32 devices in a mesh: blk: 8 (over z, y), plane: 4 (over x, core).
Axes of the slice: x: 2, y: 2, z: 4, core: 2. Of those that a mesh axis runs over, the one named last changes fastest.
Arguments:
- tiles: bfloat16 [128, 24, 128, 128], P(('blk', 'plane')), may hold values from -0.25 to 0.25
- tile_cols: int32 [128, 24], P(('blk', 'plane')), may hold values from 0 to 511
- tile_count: int32 [128], P(('blk', 'plane')), may hold values from 18 to 24, as said below
- u_start: float32 [16384], P(('blk', 'plane')), may hold values from -0.046875 to 0.046875
- v_start: float32 [65536], P(('blk', 'plane')), may hold values from -0.0234375 to 0.0234375
- beta_start: float32 [1], replicated, may hold values from 0.5 to 1.5
- left_basis: float32 [16384, 128], P(('blk', 'plane')), may hold values from -0.046875 to 0.046875
- right_basis: float32 [65536, 128], P(('blk', 'plane')), may hold values from -0.0234375 to 0.0234375
Outputs:
- left_vectors: float32 [1, 16384], P(None, ('blk', 'plane'))
- right_vectors: float32 [1, 65536], P(None, ('blk', 'plane'))
- coefficients: float32 [2], replicated
The draws below stay inside these ranges and needn't reach their ends.
Inputs may be any that keep to these rules, and one draw needn't show every extreme that they name: `tile_count`: slots at and after a row block's count are padding; some row block uses all 24 slots.
All inputs are finite; a program needn't handle non-finite values.
Results may differ from the reference program's by a relative error of at most 0.00055.
The reference program's roundings to bfloat16 on the way count: a program that leaves them out, or rounds other values in their place, can miss the bound.
Values may be sent and summed in bfloat16 or wider, within the bound.
A program may use at most 64 MiB of HBM per device.

```python
import jax
import jax.numpy as jnp
from jax import lax

N = 65536
NT = 512
SLOTS = 24
KB = 128
ITERS = 1
BLOCKS = 128
ROWS = 16384


def draw_tile_count(key, part):
    counts = jax.random.randint(key, (BLOCKS,), max(1, 3 * SLOTS // 4), SLOTS + 1).astype(jnp.int32)
    return counts.at[0].set(SLOTS)


def plant(drawn, own_key, smallest, top_value):
    dims = drawn.shape
    spot = [jax.random.randint(jax.random.fold_in(own_key, axis), (), 0, dims[axis]) for axis in range(len(dims))]
    drawn = drawn.at[tuple(spot)].set(smallest)
    longest = dims.index(max(dims))
    spot[longest] = (spot[longest] + 1) % dims[longest]
    return drawn.at[tuple(spot)].set(top_value)


def block_scale(stream_key, extent, cuts, low, largest):
    level, own = 1.0, jax.random.fold_in(stream_key, 6)
    for position, shards_of in cuts:
        draws = jnp.exp(jax.random.uniform(jax.random.fold_in(own, position), (shards_of,), jnp.float32, low / len(cuts), largest / len(cuts)))
        level = level * jnp.repeat(draws, extent[position] // shards_of).reshape([-1 if axis == position else 1 for axis in range(len(extent))])
    return level


def centred(rng, shape, spread, limit, shards=(), kind=jnp.bfloat16):
    drawn = spread * jax.random.normal(rng, shape, jnp.float32)
    if shards:
        drawn = drawn * block_scale(rng, shape, shards, -0.22, 0.18)
    return jnp.clip(drawn, -limit, limit).astype(kind)


def setup_inputs(seed: int = 0) -> dict:
    key_of = jax.random.split(jax.random.key(seed), 9)
    tiles = centred(key_of[0], (BLOCKS, SLOTS, 128, 128), (ROWS * SLOTS * 112 // N) ** -0.5, 0.25, ((0, 32),))
    tile_cols = plant(jax.random.randint(key_of[1], (BLOCKS, SLOTS), 0, NT), jax.random.fold_in(key_of[1], 1), 0, NT - 1).astype(jnp.int32)
    tile_count = draw_tile_count(jax.random.fold_in(key_of[8], 71), 0)
    u_start = centred(key_of[3], (ROWS,), ROWS ** -0.5, 0.046875, ((0, 32),), jnp.float32)
    v_start = centred(key_of[4], (N,), N ** -0.5, 0.0234375, ((0, 32),), jnp.float32)
    beta_start = jnp.clip(jax.random.uniform(key_of[5], (1,), jnp.float32, 0.5, 1.5), 0.5, 1.5)
    left_basis = centred(key_of[6], (ROWS, KB), ROWS ** -0.5, 0.046875, ((0, 32),), jnp.float32)
    right_basis = centred(key_of[7], (N, KB), N ** -0.5, 0.0234375, ((0, 32),), jnp.float32)
    return dict(tiles=tiles, tile_cols=tile_cols, tile_count=tile_count, u_start=u_start, v_start=v_start, beta_start=beta_start, left_basis=left_basis, right_basis=right_basis)


def project_twice(vec, basis):
    high = lax.Precision.HIGHEST
    first = jnp.dot(vec, basis, precision=high)
    vec = vec - jnp.dot(basis, first, precision=high)
    second = jnp.dot(vec, basis, precision=high)
    vec = vec - jnp.dot(basis, second, precision=high)
    norm = jnp.sqrt(jnp.sum(vec * vec) + 1e-06)
    return (vec / norm, norm)

def reference(tiles, tile_cols, tile_count, u_start, v_start, beta_start, left_basis, right_basis):
    high = lax.Precision.HIGHEST
    live = (jnp.arange(SLOTS, dtype=jnp.int32)[None, :] < tile_count[:, None]).astype(jnp.float32)

    def forward(rounded):
        table = rounded.reshape(-1, 128)

        def single(items):
            block, cols, weight = items
            picked = table[cols].astype(jnp.float32)
            values = jnp.einsum('sij,sj->si', block.astype(jnp.float32), picked, precision=high)
            return lax.optimization_barrier(jnp.sum(values * weight[:, None], axis=0))
        return lax.map(single, (tiles, tile_cols, live)).reshape(-1)

    def backward(rounded):
        table = rounded.reshape(-1, 128)

        def single(items):
            block, row, weight = items
            values = jnp.einsum('sij,i->sj', block.astype(jnp.float32), row.astype(jnp.float32), precision=high)
            return values * weight[:, None]
        contrib = lax.map(single, (tiles, table, live)).reshape(-1, 128)
        summed = jax.ops.segment_sum(contrib, tile_cols.reshape(-1), num_segments=N // 128)
        return summed.reshape(-1)
    vec_right = v_start
    vec_left = u_start
    beta = beta_start[0]
    lefts, rights, coefs = ([], [], [])
    for step in range(ITERS):
        forward_out = forward(vec_right.astype(jnp.bfloat16))
        vec_left, alpha = project_twice(forward_out - beta * vec_left, left_basis)
        back_out = backward(vec_left.astype(jnp.bfloat16))
        vec_right, beta = project_twice(back_out - alpha * vec_right, right_basis)
        lefts.append(vec_left * jnp.sqrt(jnp.float32(ROWS)))
        rights.append(vec_right * jnp.sqrt(jnp.float32(N)))
        coefs.append(alpha)
        coefs.append(beta)
    return (jnp.stack(lefts), jnp.stack(rights), jnp.stack(coefs))
```

```python
import functools
import math

import jax
import jax.numpy as jnp
from jax import lax
from jax.experimental import pallas as pl
from jax.experimental.pallas import tpu as pltpu
from jax.sharding import PartitionSpec as P

AXES = ("blk", "plane")
LANES = 128
SUB = 8
NT_DIMS = (((1,), (1,)), ((), ()))
MAIN_VMEM = 67043328
MESH = pl.DeviceIdType.MESH
UNROLL_DEVICES = 32


def far_first(blks, planes):
    masks = [(b, p) for b in range(blks) for p in range(planes) if b or p]
    weight = lambda m: m[0] // 2 + m[0] % 2 + m[1] // 2 + 0.3 * (m[1] % 2)
    return sorted(masks, key=weight, reverse=True)


def flips(index, size):
    steps = []
    bit = 1
    while bit < size:
        steps.append(bit * (1 - 2 * lax.rem(index // bit, 2)))
        bit *= 2
    values = []
    for mask in range(size):
        value = index
        for k, step in enumerate(steps):
            if mask >> k & 1:
                value = value + step
        values.append(value)
    return values


def steps_kernel(
    blks,
    planes,
    own_tiles,
    left_scale,
    right_scale,
    beta_hbm,
    count_hbm,
    cols_hbm,
    u_hbm,
    v_hbm,
    tiles_hbm,
    left_hbm,
    right_hbm,
    out_ref,
    beta_s,
    count_s,
    cols_s,
    cols_v,
    u_scr,
    v_scr,
    tiles,
    left,
    right,
    left_t,
    right_t,
    v_send,
    v_all,
    v_table,
    cols_rows,
    put_hot,
    shift_scr,
    p_scr,
    contrib,
    gram_send,
    gram_recv,
    gram_sum,
    gram_all,
    gram_scr,
    dot_send,
    dot_recv,
    part_send,
    part_recv,
    copy_sem,
    send_sem,
    recv_sem,
):
    devices = blks * planes
    blocks, slots = cols_v.shape
    keep = left.shape[1]
    me_blk, me_plane = lax.axis_index("blk"), lax.axis_index("plane")
    me = me_blk * planes + me_plane
    chunks, rows = gram_send.shape[1:3]
    pad_tiles = v_send.shape[0]
    part_rows = part_send.shape[1]
    entries = contrib.shape[0]
    stride = entries // blocks
    two_power = blks & (blks - 1) == 0 and planes & (planes - 1) == 0
    unrolled = two_power and devices <= UNROLL_DEVICES
    if unrolled:
        blk_of, plane_of = flips(me_blk, blks), flips(me_plane, planes)
        order = far_first(blks, planes)

    def each_other(act):
        if unrolled:
            for b, p in order:
                act(blk_of[b] * planes + plane_of[p], (blk_of[b], plane_of[p]))
            return

        def body(step, carry):
            other = lax.rem(me + step, devices)
            act(other, (other // planes, lax.rem(other, planes)))
            return carry

        lax.fori_loop(1, devices, body, 0)

    barrier = pltpu.get_barrier_semaphore()
    each_other(
        lambda other, place: pl.semaphore_signal(
            barrier, inc=1, device_id=place, device_id_type=MESH
        )
    )

    pairs = (
        (v_hbm, v_scr),
        (cols_hbm, cols_v),
        (count_hbm, count_s),
        (cols_hbm, cols_s),
        (beta_hbm, beta_s),
        (u_hbm, u_scr),
        (left_hbm, left),
        (right_hbm, right),
        (tiles_hbm, tiles),
    )
    loads = [pltpu.make_async_copy(a, b, copy_sem.at[i]) for i, (a, b) in enumerate(pairs)]
    for load in loads:
        load.start()
    v_load, cols_load, count_load, index_load, beta_load, u_load, left_load, right_load, tiles_load = loads

    def send_all(phase, source, landing):
        each_other(
            lambda other, place: pltpu.make_async_remote_copy(
                src_ref=source(other),
                dst_ref=landing.at[me],
                send_sem=send_sem.at[phase],
                recv_sem=recv_sem.at[phase],
                device_id=place,
                device_id_type=MESH,
            ).start()
        )

    def wait_all(sem, phase, landing):
        most = landing.at[pl.ds(0, devices - 1)]
        pltpu.make_async_copy(most, most, sem.at[phase]).wait()

    eye = lax.broadcasted_iota(jnp.int32, (LANES, LANES), 0) == lax.broadcasted_iota(
        jnp.int32, (LANES, LANES), 1
    )

    def to_col(row):
        return jnp.sum(jnp.where(eye, row, 0.0), axis=1, keepdims=True)

    def to_row(col):
        return jnp.sum(jnp.where(eye, col, 0.0), axis=0, keepdims=True)

    def fold(block):
        return jnp.sum(block.reshape(LANES // SUB, SUB, LANES), axis=0)

    v_load.wait()
    rounded = v_scr[...]
    if pad_tiles > own_tiles:
        rounded = jnp.concatenate(
            [rounded, jnp.zeros((pad_tiles - own_tiles, LANES), jnp.float32)], axis=0
        )
    rounded = rounded.astype(jnp.bfloat16)
    v_send[...] = rounded
    v_all[me] = rounded
    v_table[devices * pad_tiles :, :] = jnp.zeros((SUB, LANES), jnp.float32)

    def start_gram(side, basis_t):
        whole = basis_t[...]
        high = whole.astype(jnp.bfloat16)
        rest = whole - high.astype(jnp.float32)
        mid = rest.astype(jnp.bfloat16)
        low = (rest - mid.astype(jnp.float32)).astype(jnp.bfloat16)

        def product(a, b):
            return lax.dot_general(a, b, NT_DIMS, preferred_element_type=jnp.float32)

        cross = product(high, mid) + product(high, low)
        gram = product(high, high) + (cross + cross.T + product(mid, mid))
        for c in range(chunks):
            gram_send[side, c] = gram[c * rows : (c + 1) * rows, :]
        gram_recv[side, me] = gram_send[side, lax.rem(me, chunks)]

    def send_gram(side, phase):
        send_all(
            phase, lambda other: gram_send.at[side, lax.rem(other, chunks)], gram_recv.at[side]
        )

    def share_gram(side, phase):
        wait_all(recv_sem, phase, gram_recv.at[side])
        mine = jnp.sum(gram_recv[side], axis=0)
        gram_sum[side] = mine
        gram_all[side, me] = mine
        send_all(phase + 1, lambda other: gram_sum.at[side], gram_all.at[side])

    def finish_gram(side, phase):
        wait_all(recv_sem, phase + 1, gram_all.at[side])
        for c in range(chunks):
            gram_scr[c * rows : (c + 1) * rows, :] = gram_all[side, c]
        return gram_scr[...]

    left_load.wait()
    for r in range(left.shape[0] // LANES):
        left_t[:, r * LANES : (r + 1) * LANES] = left[r * LANES : (r + 1) * LANES, :].T
    start_gram(0, left_t)

    pl.semaphore_wait(barrier, devices - 1)
    send_all(0, lambda other: v_send, v_all)
    send_gram(0, 1)

    cols_load.wait()
    count_load.wait()
    index_load.wait()
    beta_load.wait()
    u_load.wait()
    cols_rows[...] = jnp.full(cols_rows.shape, -1.0, jnp.float32)
    for r in range(blocks):
        row = cols_v[r : r + 1, :]
        alive = lax.broadcasted_iota(jnp.int32, (1, slots), 1) < count_s[r]
        cols_rows[r : r + 1, 0:slots] = jnp.where(alive, row, -1).astype(jnp.float32)
    lane = lax.broadcasted_iota(jnp.int32, (1, entries), 1)
    line = jnp.full((1, entries), -1.0, jnp.float32)
    for r in range(blocks):
        row = cols_rows[r : r + 1, :]
        if r:
            row = pltpu.roll(row, r * stride, 1)
        line = jnp.where((lane >= r * stride) & (lane < r * stride + slots), row, line)
    whole = line.astype(jnp.int32)
    put_row = jnp.where(whole < 0, -1, whole // own_tiles * part_rows + whole % own_tiles)
    hot = jnp.where(
        lax.broadcasted_iota(jnp.int32, (put_hot.shape[0], entries), 0) == put_row, 1.0, 0.0
    ).astype(jnp.bfloat16)
    put_hot[:, 0:entries] = hot
    put_hot[:, entries:] = hot
    contrib[...] = jnp.zeros_like(contrib)
    beta = beta_s[0]
    for r in range(blocks):
        shift_scr[r] = jnp.where(eye, -beta * u_scr[r : r + 1, :], 0.0)

    right_load.wait()
    for t in range(own_tiles):
        right_t[:, t * LANES : (t + 1) * LANES] = right[t * LANES : (t + 1) * LANES, :].T
    start_gram(1, right_t)
    tiles_load.wait()

    wait_all(recv_sem, 0, v_all)
    v_table[0 : devices * pad_tiles, :] = (
        v_all[...].reshape(devices * pad_tiles, LANES).astype(jnp.float32)
    )
    dots = jnp.zeros((SUB, LANES), jnp.float32)
    square = jnp.zeros((SUB, LANES), jnp.float32)
    for r in range(blocks):
        total = shift_scr[r]
        for s in range(slots):
            col = cols_s[r, s]
            if pad_tiles != own_tiles:
                col = col // own_tiles * pad_tiles + lax.rem(col, own_tiles)
            col = jnp.where(s < count_s[r], col, devices * pad_tiles)
            total = total + tiles[r, s].astype(jnp.float32) * v_table[pl.ds(col, 1), :]
        p_col = jnp.broadcast_to(jnp.sum(total, axis=1, keepdims=True), (LANES, LANES))
        p_scr[r] = p_col
        dots = dots + fold(left[r * LANES : (r + 1) * LANES, :] * p_col)
        square = square + fold(p_col * p_col)

    def start_dots(side, both):
        dot_send[side] = both
        dot_recv[side, me] = both
        send_all(3 + side, lambda other: dot_send.at[side], dot_recv.at[side])

    def finish_dots(side, phase):
        wait_all(recv_sem, 3 + side, dot_recv.at[side])
        both = jnp.sum(dot_recv[side], axis=0)
        first, square = both[0:1, :], both[1:2, :]
        gram = finish_gram(side, phase)
        twice = jnp.where(eye, 2.0, 0.0) - gram
        coef = jnp.sum(twice * first, axis=1, keepdims=True)
        coef_row = to_row(coef)
        spread = jnp.sum(gram * coef, axis=0, keepdims=True)
        change = jnp.sum(coef_row * (spread - 2.0 * first), axis=1, keepdims=True)
        return coef, coef_row, jnp.sqrt(square[0:1, 0:1] + change + 1e-06)

    start_dots(
        0,
        jnp.concatenate(
            [jnp.sum(dots, axis=0, keepdims=True), jnp.sum(square, axis=0, keepdims=True)], axis=0
        ),
    )
    share_gram(0, 1)
    send_gram(1, 6)

    coef, coef_row, alpha = finish_dots(0, 1)
    inverse = 1.0 / alpha

    for r in range(blocks):
        fix = jnp.sum(left[r * LANES : (r + 1) * LANES, :] * coef_row, axis=1, keepdims=True)
        p_scr[r] = (p_scr[r] - fix) * inverse

    for r in range(blocks):
        col = p_scr[r].astype(jnp.bfloat16).astype(jnp.float32)
        for g in range(0, slots, SUB):
            lines = [
                jnp.sum(fold(tiles[r, s].astype(jnp.float32) * col), axis=0, keepdims=True)
                for s in range(g, min(g + SUB, slots))
            ]
            contrib[r * stride + g : r * stride + g + len(lines), :] = jnp.concatenate(lines, axis=0)
    whole = contrib[...]
    high = whole.astype(jnp.bfloat16)
    low = (whole - high.astype(jnp.float32)).astype(jnp.bfloat16)
    spread = jnp.dot(
        put_hot[...], jnp.concatenate([high, low], axis=0), preferred_element_type=jnp.float32
    )
    part_send[...] = spread.reshape(devices, part_rows, LANES)
    part_recv[me] = part_send[me]
    send_all(5, lambda other: part_send.at[other], part_recv)
    share_gram(1, 6)
    for r in range(blocks):
        out_ref[own_tiles + r : own_tiles + r + 1, :] = to_row(p_scr[r]) * left_scale
    wait_all(recv_sem, 5, part_recv)
    own = jnp.sum(part_recv[...], axis=0)
    r_vec = own[0:own_tiles, :] - alpha * v_scr[...]

    total = jnp.zeros((keep, LANES), jnp.float32)
    for t in range(own_tiles):
        total = total + right_t[:, t * LANES : (t + 1) * LANES] * r_vec[t : t + 1, :]
    dots = to_row(jnp.sum(total, axis=1, keepdims=True))
    square = jnp.sum(r_vec * r_vec, keepdims=True)
    start_dots(1, jnp.concatenate([dots, jnp.broadcast_to(square, (1, LANES))], axis=0))
    coef, coef_row, beta_new = finish_dots(1, 6)
    place = lax.broadcasted_iota(jnp.int32, (1, LANES), 1)
    out_ref[own_tiles + blocks : own_tiles + blocks + 1, :] = jnp.where(
        place == 0, alpha, beta_new
    )
    inverse = right_scale / beta_new
    for t in range(own_tiles):
        fix = jnp.sum(right_t[:, t * LANES : (t + 1) * LANES] * coef, axis=0, keepdims=True)
        out_ref[t : t + 1, :] = (r_vec[t : t + 1, :] - fix) * inverse

    wait_all(send_sem, 0, v_all)
    for phase, side in ((1, 0), (6, 1)):
        wait_all(send_sem, phase, gram_recv.at[side])
        wait_all(send_sem, phase + 1, gram_all.at[side])
    wait_all(send_sem, 3, dot_recv.at[0])
    wait_all(send_sem, 4, dot_recv.at[1])
    wait_all(send_sem, 5, part_recv)


def place_kernel(own_tiles, blocks, packed, out_left, out_right, out_coef):
    for r in range(blocks):
        out_left[:, r * LANES : (r + 1) * LANES] = packed[own_tiles + r : own_tiles + r + 1, :]
    for t in range(own_tiles):
        out_right[:, t * LANES : (t + 1) * LANES] = packed[t : t + 1, :]
    out_coef[...] = packed[own_tiles + blocks, 0:2]


def on_device(tiles, tile_cols, tile_count, u_start, v_start, beta_start, left_basis, right_basis):
    blks, planes = lax.axis_size("blk"), lax.axis_size("plane")
    devices = blks * planes
    blocks, slots = tile_cols.shape
    own_tiles = v_start.shape[0] // LANES
    left_rows, keep = left_basis.shape
    right_rows = right_basis.shape[0]
    pad_tiles = -(-own_tiles // 16) * 16
    part_rows = -(-own_tiles // 8) * 8
    rows = max(4, keep // devices)
    chunks = keep // rows
    stride = -(-slots // 8) * 8
    while (blocks * stride) % LANES:
        stride += 8
    entries = blocks * stride
    f32, bf16, i32 = jnp.float32, jnp.bfloat16, jnp.int32
    vmem = pl.BlockSpec(memory_space=pltpu.VMEM)
    hbm = pl.BlockSpec(memory_space=pl.ANY)
    packed = pl.pallas_call(
        functools.partial(
            steps_kernel,
            blks,
            planes,
            own_tiles,
            math.sqrt(left_rows * devices),
            math.sqrt(right_rows * devices),
        ),
        out_shape=jax.ShapeDtypeStruct((own_tiles + blocks + 1, LANES), f32),
        in_specs=[hbm] * 8,
        out_specs=vmem,
        scratch_shapes=[
            pltpu.SMEM((1,), f32),
            pltpu.SMEM((blocks,), i32),
            pltpu.SMEM((blocks, slots), i32),
            pltpu.VMEM((blocks, slots), i32),
            pltpu.VMEM((blocks, LANES), f32),
            pltpu.VMEM((own_tiles, LANES), f32),
            pltpu.VMEM(tiles.shape, bf16),
            pltpu.VMEM(left_basis.shape, f32),
            pltpu.VMEM(right_basis.shape, f32),
            pltpu.VMEM((keep, left_rows), f32),
            pltpu.VMEM((keep, right_rows), f32),
            pltpu.VMEM((pad_tiles, LANES), bf16),
            pltpu.VMEM((devices, pad_tiles, LANES), bf16),
            pltpu.VMEM((devices * pad_tiles + SUB, LANES), f32),
            pltpu.VMEM((-(-blocks // 8) * 8, entries), f32),
            pltpu.VMEM((devices * part_rows, 2 * entries), bf16),
            pltpu.VMEM((blocks, LANES, LANES), f32),
            pltpu.VMEM((blocks, LANES, LANES), f32),
            pltpu.VMEM((entries, LANES), f32),
            pltpu.VMEM((2, chunks, rows, keep), f32),
            pltpu.VMEM((2, devices, rows, keep), f32),
            pltpu.VMEM((2, rows, keep), f32),
            pltpu.VMEM((2, devices, rows, keep), f32),
            pltpu.VMEM((keep, keep), f32),
            pltpu.VMEM((2, 2, keep), f32),
            pltpu.VMEM((2, devices, 2, keep), f32),
            pltpu.VMEM((devices, part_rows, LANES), f32),
            pltpu.VMEM((devices, part_rows, LANES), f32),
            pltpu.SemaphoreType.DMA((9,)),
            pltpu.SemaphoreType.DMA((8,)),
            pltpu.SemaphoreType.DMA((8,)),
        ],
        compiler_params=pltpu.CompilerParams(
            collective_id=0, has_side_effects=True, vmem_limit_bytes=MAIN_VMEM
        ),
    )(
        beta_start,
        tile_count,
        tile_cols,
        u_start.reshape(blocks, LANES),
        v_start.reshape(own_tiles, LANES),
        tiles,
        left_basis,
        right_basis,
    )
    return pl.pallas_call(
        functools.partial(place_kernel, own_tiles, blocks),
        out_shape=(
            jax.ShapeDtypeStruct((1, left_rows), f32),
            jax.ShapeDtypeStruct((1, right_rows), f32),
            jax.ShapeDtypeStruct((2,), f32),
        ),
        in_specs=[vmem],
        out_specs=(vmem, vmem, vmem),
        compiler_params=pltpu.CompilerParams(vmem_limit_bytes=MAIN_VMEM),
    )(packed)


def solution(mesh):
    placed = (
        P(AXES, None, None, None),
        P(AXES, None),
        P(AXES),
        P(AXES),
        P(AXES),
        P(),
        P(AXES, None),
        P(AXES, None),
    )
    return jax.shard_map(
        on_device,
        mesh=mesh,
        in_specs=placed,
        out_specs=(P(None, AXES), P(None, AXES), P()),
        check_vma=False,
    )
```

```python
import functools
import math

import jax
import jax.numpy as jnp
from jax import lax
from jax.experimental import pallas as pl
from jax.experimental.pallas import tpu as pltpu
from jax.sharding import PartitionSpec as P

AXES = ("blk", "plane")
LANES = 128
SUB = 8
NT_DIMS = (((1,), (1,)), ((), ()))
MAIN_VMEM = 67043328
MESH = pl.DeviceIdType.MESH
UNROLL_DEVICES = 32


def far_first(blks, planes):
    masks = [(b, p) for b in range(blks) for p in range(planes) if b or p]
    weight = lambda m: m[0] // 2 + m[0] % 2 + m[1] // 2 + 0.3 * (m[1] % 2)
    return sorted(masks, key=weight, reverse=True)


def flips(index, size):
    steps = []
    bit = 1
    while bit < size:
        steps.append(bit * (1 - 2 * lax.rem(index // bit, 2)))
        bit *= 2
    values = []
    for mask in range(size):
        value = index
        for k, step in enumerate(steps):
            if mask >> k & 1:
                value = value + step
        values.append(value)
    return values


def steps_kernel(
    blks,
    planes,
    own_tiles,
    left_scale,
    right_scale,
    beta_hbm,
    count_hbm,
    cols_hbm,
    u_hbm,
    v_hbm,
    tiles_hbm,
    left_hbm,
    right_hbm,
    out_ref,
    beta_s,
    count_s,
    cols_s,
    cols_v,
    u_scr,
    v_scr,
    tiles,
    left,
    right,
    left_t,
    right_t,
    v_send,
    v_all,
    v_table,
    cols_rows,
    put_hot,
    shift_scr,
    p_scr,
    contrib,
    gram_send,
    gram_recv,
    gram_sum,
    gram_all,
    gram_scr,
    dot_send,
    dot_recv,
    part_send,
    part_recv,
    copy_sem,
    send_sem,
    recv_sem,
):
    devices = blks * planes
    blocks, slots = cols_v.shape
    keep = left.shape[1]
    me_blk, me_plane = lax.axis_index("blk"), lax.axis_index("plane")
    me = me_blk * planes + me_plane
    chunks, rows = gram_send.shape[1:3]
    pad_tiles = v_send.shape[0]
    words = part_send.shape[1] - 1
    part_rows = 2 * words
    entries = contrib.shape[0]
    stride = entries // blocks
    two_power = blks & (blks - 1) == 0 and planes & (planes - 1) == 0
    unrolled = two_power and devices <= UNROLL_DEVICES
    if unrolled:
        blk_of, plane_of = flips(me_blk, blks), flips(me_plane, planes)
        order = far_first(blks, planes)

    def each_other(act):
        if unrolled:
            for b, p in order:
                act(blk_of[b] * planes + plane_of[p], (blk_of[b], plane_of[p]))
            return

        def body(step, carry):
            other = lax.rem(me + step, devices)
            act(other, (other // planes, lax.rem(other, planes)))
            return carry

        lax.fori_loop(1, devices, body, 0)

    barrier = pltpu.get_barrier_semaphore()
    each_other(
        lambda other, place: pl.semaphore_signal(
            barrier, inc=1, device_id=place, device_id_type=MESH
        )
    )

    pairs = (
        (v_hbm, v_scr),
        (cols_hbm, cols_v),
        (count_hbm, count_s),
        (cols_hbm, cols_s),
        (beta_hbm, beta_s),
        (u_hbm, u_scr),
        (left_hbm, left),
        (right_hbm, right),
        (tiles_hbm, tiles),
    )
    loads = [pltpu.make_async_copy(a, b, copy_sem.at[i]) for i, (a, b) in enumerate(pairs)]
    for load in loads:
        load.start()
    v_load, cols_load, count_load, index_load, beta_load, u_load, left_load, right_load, tiles_load = loads

    def send_all(phase, source, landing):
        each_other(
            lambda other, place: pltpu.make_async_remote_copy(
                src_ref=source(other),
                dst_ref=landing.at[me],
                send_sem=send_sem.at[phase],
                recv_sem=recv_sem.at[phase],
                device_id=place,
                device_id_type=MESH,
            ).start()
        )

    def wait_all(sem, phase, landing):
        most = landing.at[pl.ds(0, devices - 1)]
        pltpu.make_async_copy(most, most, sem.at[phase]).wait()

    eye = lax.broadcasted_iota(jnp.int32, (LANES, LANES), 0) == lax.broadcasted_iota(
        jnp.int32, (LANES, LANES), 1
    )

    def to_col(row):
        return jnp.sum(jnp.where(eye, row, 0.0), axis=1, keepdims=True)

    def to_row(col):
        return jnp.sum(jnp.where(eye, col, 0.0), axis=0, keepdims=True)

    def fold(block):
        return jnp.sum(block.reshape(LANES // SUB, SUB, LANES), axis=0)

    v_load.wait()
    rounded = v_scr[...]
    if pad_tiles > own_tiles:
        rounded = jnp.concatenate(
            [rounded, jnp.zeros((pad_tiles - own_tiles, LANES), jnp.float32)], axis=0
        )
    rounded = rounded.astype(jnp.bfloat16)
    v_send[...] = rounded
    v_all[me] = rounded
    v_table[devices * pad_tiles :, :] = jnp.zeros((SUB, LANES), jnp.float32)

    def start_gram(side, basis_t):
        whole = basis_t[...]
        high = whole.astype(jnp.bfloat16)
        rest = whole - high.astype(jnp.float32)
        mid = rest.astype(jnp.bfloat16)
        low = (rest - mid.astype(jnp.float32)).astype(jnp.bfloat16)

        def product(a, b):
            return lax.dot_general(a, b, NT_DIMS, preferred_element_type=jnp.float32)

        cross = product(high, mid) + product(high, low)
        gram = product(high, high) + (cross + cross.T + product(mid, mid))
        for c in range(chunks):
            gram_send[side, c] = gram[c * rows : (c + 1) * rows, :]
        gram_recv[side, me] = gram_send[side, lax.rem(me, chunks)]

    def send_gram(side, phase):
        send_all(
            phase, lambda other: gram_send.at[side, lax.rem(other, chunks)], gram_recv.at[side]
        )

    def share_gram(side, phase):
        wait_all(recv_sem, phase, gram_recv.at[side])
        mine = jnp.sum(gram_recv[side], axis=0)
        gram_sum[side] = mine
        gram_all[side, me] = mine
        send_all(phase + 1, lambda other: gram_sum.at[side], gram_all.at[side])

    def finish_gram(side, phase):
        wait_all(recv_sem, phase + 1, gram_all.at[side])
        for c in range(chunks):
            gram_scr[c * rows : (c + 1) * rows, :] = gram_all[side, c]
        return gram_scr[...]

    left_load.wait()
    for r in range(left.shape[0] // LANES):
        left_t[:, r * LANES : (r + 1) * LANES] = left[r * LANES : (r + 1) * LANES, :].T
    start_gram(0, left_t)

    pl.semaphore_wait(barrier, devices - 1)
    send_all(0, lambda other: v_send, v_all)
    send_gram(0, 1)

    cols_load.wait()
    count_load.wait()
    index_load.wait()
    beta_load.wait()
    u_load.wait()
    cols_rows[...] = jnp.full(cols_rows.shape, -1.0, jnp.float32)
    for r in range(blocks):
        row = cols_v[r : r + 1, :]
        alive = lax.broadcasted_iota(jnp.int32, (1, slots), 1) < count_s[r]
        cols_rows[r : r + 1, 0:slots] = jnp.where(alive, row, -1).astype(jnp.float32)
    lane = lax.broadcasted_iota(jnp.int32, (1, entries), 1)
    line = jnp.full((1, entries), -1.0, jnp.float32)
    for r in range(blocks):
        row = cols_rows[r : r + 1, :]
        if r:
            row = pltpu.roll(row, r * stride, 1)
        line = jnp.where((lane >= r * stride) & (lane < r * stride + slots), row, line)
    whole = line.astype(jnp.int32)
    put_row = jnp.where(whole < 0, -1, whole // own_tiles * part_rows + whole % own_tiles)
    hot = jnp.where(
        lax.broadcasted_iota(jnp.int32, (put_hot.shape[0], entries), 0) == put_row, 1.0, 0.0
    ).astype(jnp.bfloat16)
    put_hot[:, 0:entries] = hot
    put_hot[:, entries:] = hot
    contrib[...] = jnp.zeros_like(contrib)
    beta = beta_s[0]
    for r in range(blocks):
        shift_scr[r] = jnp.where(eye, -beta * u_scr[r : r + 1, :], 0.0)

    right_load.wait()
    for t in range(own_tiles):
        right_t[:, t * LANES : (t + 1) * LANES] = right[t * LANES : (t + 1) * LANES, :].T
    start_gram(1, right_t)
    tiles_load.wait()

    wait_all(recv_sem, 0, v_all)
    v_table[0 : devices * pad_tiles, :] = (
        v_all[...].reshape(devices * pad_tiles, LANES).astype(jnp.float32)
    )
    dots = jnp.zeros((SUB, LANES), jnp.float32)
    square = jnp.zeros((SUB, LANES), jnp.float32)
    for r in range(blocks):
        total = shift_scr[r]
        for s in range(slots):
            col = cols_s[r, s]
            if pad_tiles != own_tiles:
                col = col // own_tiles * pad_tiles + lax.rem(col, own_tiles)
            col = jnp.where(s < count_s[r], col, devices * pad_tiles)
            total = total + tiles[r, s].astype(jnp.float32) * v_table[pl.ds(col, 1), :]
        p_col = jnp.broadcast_to(jnp.sum(total, axis=1, keepdims=True), (LANES, LANES))
        p_scr[r] = p_col
        dots = dots + fold(left[r * LANES : (r + 1) * LANES, :] * p_col)
        square = square + fold(p_col * p_col)

    def start_dots(side, both):
        dot_send[side] = both
        dot_recv[side, me] = both
        send_all(3 + side, lambda other: dot_send.at[side], dot_recv.at[side])

    def finish_dots(side, phase):
        wait_all(recv_sem, 3 + side, dot_recv.at[side])
        both = jnp.sum(dot_recv[side], axis=0)
        first, square = both[0:1, :], both[1:2, :]
        gram = finish_gram(side, phase)
        twice = jnp.where(eye, 2.0, 0.0) - gram
        coef = jnp.sum(twice * first, axis=1, keepdims=True)
        coef_row = to_row(coef)
        spread = jnp.sum(gram * coef, axis=0, keepdims=True)
        change = jnp.sum(coef_row * (spread - 2.0 * first), axis=1, keepdims=True)
        return coef, coef_row, jnp.sqrt(square[0:1, 0:1] + change + 1e-06)

    start_dots(
        0,
        jnp.concatenate(
            [jnp.sum(dots, axis=0, keepdims=True), jnp.sum(square, axis=0, keepdims=True)], axis=0
        ),
    )
    share_gram(0, 1)
    send_gram(1, 6)

    coef, coef_row, alpha = finish_dots(0, 1)
    inverse = 1.0 / alpha

    for r in range(blocks):
        fix = jnp.sum(left[r * LANES : (r + 1) * LANES, :] * coef_row, axis=1, keepdims=True)
        p_scr[r] = (p_scr[r] - fix) * inverse

    for r in range(blocks):
        col = p_scr[r].astype(jnp.bfloat16).astype(jnp.float32)
        for g in range(0, slots, SUB):
            lines = [
                jnp.sum(fold(tiles[r, s].astype(jnp.float32) * col), axis=0, keepdims=True)
                for s in range(g, min(g + SUB, slots))
            ]
            contrib[r * stride + g : r * stride + g + len(lines), :] = jnp.concatenate(lines, axis=0)
    whole = contrib[...]
    high = whole.astype(jnp.bfloat16)
    low = (whole - high.astype(jnp.float32)).astype(jnp.bfloat16)
    spread = jnp.dot(
        put_hot[...], jnp.concatenate([high, low], axis=0), preferred_element_type=jnp.float32
    )
    parts = spread.reshape(devices, part_rows, LANES)
    top = jnp.maximum(jnp.max(jnp.abs(parts), axis=1, keepdims=True), 1e-30)
    power = jnp.floor(jnp.log2(top)) - 14.0
    whole = jnp.minimum(jnp.round(parts * jnp.exp2(-power)), 32767.0).astype(jnp.int32)
    part_send[:, 0:words, :] = lax.shift_left(whole[:, 0:words, :], 16) | (
        whole[:, words:, :] & 0xFFFF
    )
    part_send[:, words:, :] = power.astype(jnp.int32)
    part_recv[me] = part_send[me]
    send_all(5, lambda other: part_send.at[other], part_recv)
    share_gram(1, 6)
    for r in range(blocks):
        out_ref[own_tiles + r : own_tiles + r + 1, :] = to_row(p_scr[r]) * left_scale
    wait_all(recv_sem, 5, part_recv)
    unit = jnp.exp2(part_recv[:, words:, :].astype(jnp.float32))
    word = part_recv[:, 0:words, :]
    halves = (lax.shift_right_arithmetic(word, 16), lax.shift_right_arithmetic(lax.shift_left(word, 16), 16))
    own = jnp.concatenate(
        [jnp.sum(half.astype(jnp.float32) * unit, axis=0) for half in halves], axis=0
    )
    r_vec = own[0:own_tiles, :] - alpha * v_scr[...]

    total = jnp.zeros((keep, LANES), jnp.float32)
    for t in range(own_tiles):
        total = total + right_t[:, t * LANES : (t + 1) * LANES] * r_vec[t : t + 1, :]
    dots = to_row(jnp.sum(total, axis=1, keepdims=True))
    square = jnp.sum(r_vec * r_vec, keepdims=True)
    start_dots(1, jnp.concatenate([dots, jnp.broadcast_to(square, (1, LANES))], axis=0))
    coef, coef_row, beta_new = finish_dots(1, 6)
    place = lax.broadcasted_iota(jnp.int32, (1, LANES), 1)
    out_ref[own_tiles + blocks : own_tiles + blocks + 1, :] = jnp.where(
        place == 0, alpha, beta_new
    )
    inverse = right_scale / beta_new
    for t in range(own_tiles):
        fix = jnp.sum(right_t[:, t * LANES : (t + 1) * LANES] * coef, axis=0, keepdims=True)
        out_ref[t : t + 1, :] = (r_vec[t : t + 1, :] - fix) * inverse

    wait_all(send_sem, 0, v_all)
    for phase, side in ((1, 0), (6, 1)):
        wait_all(send_sem, phase, gram_recv.at[side])
        wait_all(send_sem, phase + 1, gram_all.at[side])
    wait_all(send_sem, 3, dot_recv.at[0])
    wait_all(send_sem, 4, dot_recv.at[1])
    wait_all(send_sem, 5, part_recv)


def place_kernel(own_tiles, blocks, packed, out_left, out_right, out_coef):
    for r in range(blocks):
        out_left[:, r * LANES : (r + 1) * LANES] = packed[own_tiles + r : own_tiles + r + 1, :]
    for t in range(own_tiles):
        out_right[:, t * LANES : (t + 1) * LANES] = packed[t : t + 1, :]
    out_coef[...] = packed[own_tiles + blocks, 0:2]


def on_device(tiles, tile_cols, tile_count, u_start, v_start, beta_start, left_basis, right_basis):
    blks, planes = lax.axis_size("blk"), lax.axis_size("plane")
    devices = blks * planes
    blocks, slots = tile_cols.shape
    own_tiles = v_start.shape[0] // LANES
    left_rows, keep = left_basis.shape
    right_rows = right_basis.shape[0]
    pad_tiles = -(-own_tiles // 16) * 16
    part_rows = -(-own_tiles // 16) * 16
    rows = max(4, keep // devices)
    chunks = keep // rows
    stride = -(-slots // 8) * 8
    while (blocks * stride) % LANES:
        stride += 8
    entries = blocks * stride
    f32, bf16, i32 = jnp.float32, jnp.bfloat16, jnp.int32
    vmem = pl.BlockSpec(memory_space=pltpu.VMEM)
    hbm = pl.BlockSpec(memory_space=pl.ANY)
    packed = pl.pallas_call(
        functools.partial(
            steps_kernel,
            blks,
            planes,
            own_tiles,
            math.sqrt(left_rows * devices),
            math.sqrt(right_rows * devices),
        ),
        out_shape=pltpu.VMEM((own_tiles + blocks + 1, LANES), f32),
        in_specs=[hbm] * 8,
        out_specs=vmem,
        scratch_shapes=[
            pltpu.SMEM((1,), f32),
            pltpu.SMEM((blocks,), i32),
            pltpu.SMEM((blocks, slots), i32),
            pltpu.VMEM((blocks, slots), i32),
            pltpu.VMEM((blocks, LANES), f32),
            pltpu.VMEM((own_tiles, LANES), f32),
            pltpu.VMEM(tiles.shape, bf16),
            pltpu.VMEM(left_basis.shape, f32),
            pltpu.VMEM(right_basis.shape, f32),
            pltpu.VMEM((keep, left_rows), f32),
            pltpu.VMEM((keep, right_rows), f32),
            pltpu.VMEM((pad_tiles, LANES), bf16),
            pltpu.VMEM((devices, pad_tiles, LANES), bf16),
            pltpu.VMEM((devices * pad_tiles + SUB, LANES), f32),
            pltpu.VMEM((-(-blocks // 8) * 8, entries), f32),
            pltpu.VMEM((devices * part_rows, 2 * entries), bf16),
            pltpu.VMEM((blocks, LANES, LANES), f32),
            pltpu.VMEM((blocks, LANES, LANES), f32),
            pltpu.VMEM((entries, LANES), f32),
            pltpu.VMEM((2, chunks, rows, keep), f32),
            pltpu.VMEM((2, devices, rows, keep), f32),
            pltpu.VMEM((2, rows, keep), f32),
            pltpu.VMEM((2, devices, rows, keep), f32),
            pltpu.VMEM((keep, keep), f32),
            pltpu.VMEM((2, 2, keep), f32),
            pltpu.VMEM((2, devices, 2, keep), f32),
            pltpu.VMEM((devices, part_rows // 2 + 1, LANES), i32),
            pltpu.VMEM((devices, part_rows // 2 + 1, LANES), i32),
            pltpu.SemaphoreType.DMA((9,)),
            pltpu.SemaphoreType.DMA((8,)),
            pltpu.SemaphoreType.DMA((8,)),
        ],
        compiler_params=pltpu.CompilerParams(
            collective_id=0, has_side_effects=True, vmem_limit_bytes=MAIN_VMEM - 512 * (-(-(own_tiles + blocks + 1) // SUB) * SUB)
        ),
    )(
        beta_start,
        tile_count,
        tile_cols,
        u_start.reshape(blocks, LANES),
        v_start.reshape(own_tiles, LANES),
        tiles,
        left_basis,
        right_basis,
    )
    return pl.pallas_call(
        functools.partial(place_kernel, own_tiles, blocks),
        out_shape=(
            jax.ShapeDtypeStruct((1, left_rows), f32),
            jax.ShapeDtypeStruct((1, right_rows), f32),
            jax.ShapeDtypeStruct((2,), f32),
        ),
        in_specs=[vmem],
        out_specs=(vmem, vmem, vmem),
        compiler_params=pltpu.CompilerParams(vmem_limit_bytes=1048576),
    )(packed)


def solution(mesh):
    placed = (
        P(AXES, None, None, None),
        P(AXES, None),
        P(AXES),
        P(AXES),
        P(AXES),
        P(),
        P(AXES, None),
        P(AXES, None),
    )
    return jax.shard_map(
        on_device,
        mesh=mesh,
        in_specs=placed,
        out_specs=(P(None, AXES), P(None, AXES), P()),
        check_vma=False,
    )
```

```python
import functools
import math

import jax
import jax.numpy as jnp
from jax import lax
from jax.experimental import pallas as pl
from jax.experimental.pallas import tpu as pltpu
from jax.sharding import PartitionSpec as P

AXES = ("blk", "plane")
LANES = 128
SUB = 8
ON_MXU = (2, 5, 7)
NT_DIMS = (((1,), (1,)), ((), ()))
MAIN_VMEM = 67043328
MESH = pl.DeviceIdType.MESH
UNROLL_DEVICES = 32


def far_first(blks, planes):
    masks = [(b, p) for b in range(blks) for p in range(planes) if b or p]
    weight = lambda m: m[0] // 2 + m[0] % 2 + m[1] // 2 + 0.3 * (m[1] % 2)
    return sorted(masks, key=weight, reverse=True)


def flips(index, size):
    steps = []
    bit = 1
    while bit < size:
        steps.append(bit * (1 - 2 * lax.rem(index // bit, 2)))
        bit *= 2
    values = []
    for mask in range(size):
        value = index
        for k, step in enumerate(steps):
            if mask >> k & 1:
                value = value + step
        values.append(value)
    return values


def steps_kernel(
    blks,
    planes,
    own_tiles,
    left_scale,
    right_scale,
    beta_hbm,
    count_hbm,
    cols_hbm,
    u_hbm,
    v_hbm,
    tiles_hbm,
    left_hbm,
    right_hbm,
    out_ref,
    beta_s,
    count_s,
    cols_s,
    cols_v,
    u_scr,
    v_scr,
    tiles,
    left,
    right,
    left_t,
    right_t,
    v_send,
    v_all,
    v_table,
    cols_rows,
    put_hot,
    shift_scr,
    p_scr,
    contrib,
    gram_send,
    gram_recv,
    gram_sum,
    gram_all,
    gram_scr,
    diagonal,
    dot_send,
    dot_recv,
    part_send,
    part_recv,
    copy_sem,
    send_sem,
    recv_sem,
):
    devices = blks * planes
    blocks, slots = cols_v.shape
    keep = left.shape[1]
    me_blk, me_plane = lax.axis_index("blk"), lax.axis_index("plane")
    me = me_blk * planes + me_plane
    chunks, rows = gram_send.shape[1:3]
    pad_tiles = v_send.shape[0]
    words = part_send.shape[1] - 1
    part_rows = 2 * words
    entries = contrib.shape[0]
    stride = entries // blocks
    two_power = blks & (blks - 1) == 0 and planes & (planes - 1) == 0
    unrolled = two_power and devices <= UNROLL_DEVICES
    if unrolled:
        blk_of, plane_of = flips(me_blk, blks), flips(me_plane, planes)
        order = far_first(blks, planes)

    def each_other(act):
        if unrolled:
            for b, p in order:
                act(blk_of[b] * planes + plane_of[p], (blk_of[b], plane_of[p]))
            return

        def body(step, carry):
            other = lax.rem(me + step, devices)
            act(other, (other // planes, lax.rem(other, planes)))
            return carry

        lax.fori_loop(1, devices, body, 0)

    barrier = pltpu.get_barrier_semaphore()
    each_other(
        lambda other, place: pl.semaphore_signal(
            barrier, inc=1, device_id=place, device_id_type=MESH
        )
    )

    pairs = (
        (v_hbm, v_scr),
        (cols_hbm, cols_v),
        (count_hbm, count_s),
        (cols_hbm, cols_s),
        (beta_hbm, beta_s),
        (u_hbm, u_scr),
        (left_hbm, left),
        (right_hbm, right),
        (tiles_hbm, tiles),
    )
    loads = [pltpu.make_async_copy(a, b, copy_sem.at[i]) for i, (a, b) in enumerate(pairs)]
    for load in loads:
        load.start()
    v_load, cols_load, count_load, index_load, beta_load, u_load, left_load, right_load, tiles_load = loads

    def send_all(phase, source, landing):
        each_other(
            lambda other, place: pltpu.make_async_remote_copy(
                src_ref=source(other),
                dst_ref=landing.at[me],
                send_sem=send_sem.at[phase],
                recv_sem=recv_sem.at[phase],
                device_id=place,
                device_id_type=MESH,
            ).start()
        )

    def wait_all(sem, phase, landing):
        most = landing.at[pl.ds(0, devices - 1)]
        pltpu.make_async_copy(most, most, sem.at[phase]).wait()

    eye = lax.broadcasted_iota(jnp.int32, (LANES, LANES), 0) == lax.broadcasted_iota(
        jnp.int32, (LANES, LANES), 1
    )

    half = keep // 2
    half_row = lax.broadcasted_iota(jnp.int32, (half, keep), 0)
    half_lane = lax.broadcasted_iota(jnp.int32, (half, keep), 1)

    def to_col(row):
        return jnp.sum(jnp.where(eye, row, 0.0), axis=1, keepdims=True)

    def to_row(col):
        return jnp.sum(jnp.where(eye, col, 0.0), axis=0, keepdims=True)

    def fold(block):
        return jnp.sum(block.reshape(LANES // SUB, SUB, LANES), axis=0)

    v_load.wait()
    rounded = v_scr[...]
    if pad_tiles > own_tiles:
        rounded = jnp.concatenate(
            [rounded, jnp.zeros((pad_tiles - own_tiles, LANES), jnp.float32)], axis=0
        )
    rounded = rounded.astype(jnp.bfloat16)
    v_send[...] = rounded
    v_all[me] = rounded
    v_table[devices * pad_tiles :, :] = jnp.zeros((SUB, LANES), jnp.float32)

    def start_gram(side, basis_t):
        whole = basis_t[...]
        high = whole.astype(jnp.bfloat16)
        rest = whole - high.astype(jnp.float32)
        mid = rest.astype(jnp.bfloat16)
        low = (rest - mid.astype(jnp.float32)).astype(jnp.bfloat16)

        def product(a, b):
            return lax.dot_general(a, b, NT_DIMS, preferred_element_type=jnp.float32)

        cross = product(high, mid) + product(high, low)
        gram = product(high, high) + (cross + cross.T + product(mid, mid))
        top, low = gram[0:half, :], pltpu.roll(gram[half:, :], half, 1)
        folded = jnp.where(half_lane >= half_row, top, low)
        for c in range(chunks):
            gram_send[side, c] = folded[c * rows : (c + 1) * rows, :]
        diagonal[side] = jnp.sum(
            jnp.where(half_lane == half_row + half, gram[half:, :], 0.0), axis=0, keepdims=True
        )
        gram_recv[side, me] = gram_send[side, lax.rem(me, chunks)]

    def send_gram(side, phase):
        send_all(
            phase, lambda other: gram_send.at[side, lax.rem(other, chunks)], gram_recv.at[side]
        )

    def share_gram(side, phase):
        wait_all(recv_sem, phase, gram_recv.at[side])
        mine = jnp.sum(gram_recv[side], axis=0)
        gram_sum[side] = mine
        gram_all[side, me] = mine
        send_all(phase + 1, lambda other: gram_sum.at[side], gram_all.at[side])

    def finish_gram(side, phase):
        wait_all(recv_sem, phase + 1, gram_all.at[side])
        for c in range(chunks):
            gram_scr[c * rows : (c + 1) * rows, :] = gram_all[side, c]
        folded = gram_scr[...]
        strict = jnp.concatenate(
            [
                jnp.where(half_lane > half_row, folded, 0.0),
                pltpu.roll(jnp.where(half_lane < half_row, folded, 0.0), half, 1),
            ],
            axis=0,
        )
        main = jnp.sum(jnp.where(half_lane == half_row, folded, 0.0), axis=0, keepdims=True)
        return strict + strict.T + jnp.where(eye, main, 0.0)

    left_load.wait()
    for r in range(left.shape[0] // LANES):
        left_t[:, r * LANES : (r + 1) * LANES] = left[r * LANES : (r + 1) * LANES, :].T
    start_gram(0, left_t)

    pl.semaphore_wait(barrier, devices - 1)
    send_all(0, lambda other: v_send, v_all)
    send_gram(0, 1)

    cols_load.wait()
    count_load.wait()
    index_load.wait()
    beta_load.wait()
    u_load.wait()
    cols_rows[...] = jnp.full(cols_rows.shape, -1.0, jnp.float32)
    for r in range(blocks):
        row = cols_v[r : r + 1, :]
        alive = lax.broadcasted_iota(jnp.int32, (1, slots), 1) < count_s[r]
        cols_rows[r : r + 1, 0:slots] = jnp.where(alive, row, -1).astype(jnp.float32)
    lane = lax.broadcasted_iota(jnp.int32, (1, entries), 1)
    line = jnp.full((1, entries), -1.0, jnp.float32)
    for r in range(blocks):
        row = cols_rows[r : r + 1, :]
        if r:
            row = pltpu.roll(row, r * stride, 1)
        line = jnp.where((lane >= r * stride) & (lane < r * stride + slots), row, line)
    whole = line.astype(jnp.int32)
    put_row = jnp.where(whole < 0, -1, whole // own_tiles * part_rows + whole % own_tiles)
    hot = jnp.where(
        lax.broadcasted_iota(jnp.int32, (put_hot.shape[0], entries), 0) == put_row, 1.0, 0.0
    ).astype(jnp.bfloat16)
    put_hot[:, 0:entries] = hot
    put_hot[:, entries:] = hot
    contrib[...] = jnp.zeros_like(contrib)
    beta = beta_s[0]
    for r in range(blocks):
        shift_scr[r] = jnp.where(eye, -beta * u_scr[r : r + 1, :], 0.0)

    right_load.wait()
    for t in range(own_tiles):
        right_t[:, t * LANES : (t + 1) * LANES] = right[t * LANES : (t + 1) * LANES, :].T
    start_gram(1, right_t)
    tiles_load.wait()

    wait_all(recv_sem, 0, v_all)
    v_table[0 : devices * pad_tiles, :] = (
        v_all[...].reshape(devices * pad_tiles, LANES).astype(jnp.float32)
    )
    dots = jnp.zeros((SUB, LANES), jnp.float32)
    square = jnp.zeros((SUB, LANES), jnp.float32)
    for r in range(blocks):
        if r == blocks - 1:
            share_gram(0, 1)
        total = shift_scr[r]
        for s in range(slots):
            col = cols_s[r, s]
            if pad_tiles != own_tiles:
                col = col // own_tiles * pad_tiles + lax.rem(col, own_tiles)
            col = jnp.where(s < count_s[r], col, devices * pad_tiles)
            total = total + tiles[r, s].astype(jnp.float32) * v_table[pl.ds(col, 1), :]
        p_col = jnp.broadcast_to(jnp.sum(total, axis=1, keepdims=True), (LANES, LANES))
        p_scr[r] = p_col
        dots = dots + fold(left[r * LANES : (r + 1) * LANES, :] * p_col)
        square = square + fold(p_col * p_col)

    def start_dots(side, dots, square):
        lane = lax.broadcasted_iota(jnp.int32, (1, keep), 1)
        both = jnp.concatenate([dots, jnp.where(lane >= half, diagonal[side], square)], axis=0)
        dot_send[side] = both
        dot_recv[side, me] = both
        send_all(3 + side, lambda other: dot_send.at[side], dot_recv.at[side])

    def finish_dots(side, phase):
        gram = finish_gram(side, phase)
        wait_all(recv_sem, 3 + side, dot_recv.at[side])
        both = jnp.sum(dot_recv[side], axis=0)
        first, square = both[0:1, :], both[1:2, 0:1]
        lane = lax.broadcasted_iota(jnp.int32, (1, keep), 1)
        gram = gram + jnp.where(eye & (lane >= half), both[1:2, :], 0.0)
        twice = jnp.where(eye, 2.0, 0.0) - gram
        coef = jnp.sum(twice * first, axis=1, keepdims=True)
        coef_row = to_row(coef)
        spread = jnp.sum(gram * coef, axis=0, keepdims=True)
        change = jnp.sum(coef_row * (spread - 2.0 * first), axis=1, keepdims=True)
        return coef, coef_row, jnp.sqrt(square + change + 1e-06)

    start_dots(
        0, jnp.sum(dots, axis=0, keepdims=True), jnp.sum(square, axis=0, keepdims=True)
    )
    send_gram(1, 6)

    coef, coef_row, alpha = finish_dots(0, 1)
    inverse = 1.0 / alpha

    for r in range(blocks):
        fix = jnp.sum(left[r * LANES : (r + 1) * LANES, :] * coef_row, axis=1, keepdims=True)
        p_scr[r] = (p_scr[r] - fix) * inverse

    spot = lax.broadcasted_iota(jnp.int32, (SUB, LANES), 0)
    for r in range(blocks):
        rounded = p_scr[r].astype(jnp.bfloat16)
        col = rounded.astype(jnp.float32)
        row = jnp.broadcast_to(to_row(col), (2 * SUB, LANES)).astype(jnp.bfloat16)
        for g in range(0, slots, SUB):
            lines = jnp.zeros((SUB, LANES), jnp.float32)
            for s in range(g, min(g + SUB, slots)):
                if s % SUB in ON_MXU:
                    line = jnp.dot(row, tiles[r, s], preferred_element_type=jnp.float32)[0:SUB, :]
                else:
                    line = jnp.sum(fold(tiles[r, s].astype(jnp.float32) * col), axis=0, keepdims=True)
                lines = jnp.where(spot == s - g, line, lines)
            contrib[r * stride + g : r * stride + g + SUB, :] = lines
    whole = contrib[...]
    high = whole.astype(jnp.bfloat16)
    low = (whole - high.astype(jnp.float32)).astype(jnp.bfloat16)
    spread = jnp.dot(
        put_hot[...], jnp.concatenate([high, low], axis=0), preferred_element_type=jnp.float32
    )
    parts = spread.reshape(devices, part_rows, LANES)
    top = jnp.maximum(jnp.max(jnp.abs(parts), axis=1, keepdims=True), 1e-30)
    power = jnp.floor(jnp.log2(top)) - 14.0
    whole = jnp.minimum(jnp.round(parts * jnp.exp2(-power)), 32767.0).astype(jnp.int32)
    part_send[:, 0:words, :] = lax.shift_left(whole[:, 0:words, :], 16) | (
        whole[:, words:, :] & 0xFFFF
    )
    part_send[:, words:, :] = power.astype(jnp.int32)
    part_recv[me] = part_send[me]
    send_all(5, lambda other: part_send.at[other], part_recv)
    for r in range(blocks):
        out_ref[own_tiles + r : own_tiles + r + 1, :] = to_row(p_scr[r]) * left_scale
    wait_all(recv_sem, 5, part_recv)
    share_gram(1, 6)
    unit = jnp.exp2(part_recv[:, words:, :].astype(jnp.float32))
    word = part_recv[:, 0:words, :]
    halves = (lax.shift_right_arithmetic(word, 16), lax.shift_right_arithmetic(lax.shift_left(word, 16), 16))
    own = jnp.concatenate(
        [jnp.sum(half.astype(jnp.float32) * unit, axis=0) for half in halves], axis=0
    )
    r_vec = own[0:own_tiles, :] - alpha * v_scr[...]

    total = jnp.zeros((keep, LANES), jnp.float32)
    for t in range(own_tiles):
        total = total + right_t[:, t * LANES : (t + 1) * LANES] * r_vec[t : t + 1, :]
    dots = to_row(jnp.sum(total, axis=1, keepdims=True))
    square = jnp.sum(r_vec * r_vec, keepdims=True)
    start_dots(1, dots, jnp.broadcast_to(square, (1, LANES)))
    coef, coef_row, beta_new = finish_dots(1, 6)
    place = lax.broadcasted_iota(jnp.int32, (1, LANES), 1)
    out_ref[own_tiles + blocks : own_tiles + blocks + 1, :] = jnp.where(
        place == 0, alpha, beta_new
    )
    inverse = right_scale / beta_new
    for t in range(own_tiles):
        fix = jnp.sum(right_t[:, t * LANES : (t + 1) * LANES] * coef, axis=0, keepdims=True)
        out_ref[t : t + 1, :] = (r_vec[t : t + 1, :] - fix) * inverse

    wait_all(send_sem, 0, v_all)
    for phase, side in ((1, 0), (6, 1)):
        wait_all(send_sem, phase, gram_recv.at[side])
        wait_all(send_sem, phase + 1, gram_all.at[side])
    wait_all(send_sem, 3, dot_recv.at[0])
    wait_all(send_sem, 4, dot_recv.at[1])
    wait_all(send_sem, 5, part_recv)


def place_kernel(own_tiles, blocks, packed, out_left, out_right, out_coef):
    for r in range(blocks):
        out_left[:, r * LANES : (r + 1) * LANES] = packed[own_tiles + r : own_tiles + r + 1, :]
    for t in range(own_tiles):
        out_right[:, t * LANES : (t + 1) * LANES] = packed[t : t + 1, :]
    out_coef[...] = packed[own_tiles + blocks, 0:2]


def on_device(tiles, tile_cols, tile_count, u_start, v_start, beta_start, left_basis, right_basis):
    blks, planes = lax.axis_size("blk"), lax.axis_size("plane")
    devices = blks * planes
    blocks, slots = tile_cols.shape
    own_tiles = v_start.shape[0] // LANES
    left_rows, keep = left_basis.shape
    right_rows = right_basis.shape[0]
    pad_tiles = -(-own_tiles // 16) * 16
    part_rows = -(-own_tiles // 16) * 16
    rows = max(2, keep // 2 // devices)
    chunks = keep // 2 // rows
    stride = -(-slots // 8) * 8
    while (blocks * stride) % LANES:
        stride += 8
    entries = blocks * stride
    f32, bf16, i32 = jnp.float32, jnp.bfloat16, jnp.int32
    vmem = pl.BlockSpec(memory_space=pltpu.VMEM)
    hbm = pl.BlockSpec(memory_space=pl.ANY)
    packed = pl.pallas_call(
        functools.partial(
            steps_kernel,
            blks,
            planes,
            own_tiles,
            math.sqrt(left_rows * devices),
            math.sqrt(right_rows * devices),
        ),
        out_shape=pltpu.VMEM((own_tiles + blocks + 1, LANES), f32),
        in_specs=[hbm] * 8,
        out_specs=vmem,
        scratch_shapes=[
            pltpu.SMEM((1,), f32),
            pltpu.SMEM((blocks,), i32),
            pltpu.SMEM((blocks, slots), i32),
            pltpu.VMEM((blocks, slots), i32),
            pltpu.VMEM((blocks, LANES), f32),
            pltpu.VMEM((own_tiles, LANES), f32),
            pltpu.VMEM(tiles.shape, bf16),
            pltpu.VMEM(left_basis.shape, f32),
            pltpu.VMEM(right_basis.shape, f32),
            pltpu.VMEM((keep, left_rows), f32),
            pltpu.VMEM((keep, right_rows), f32),
            pltpu.VMEM((pad_tiles, LANES), bf16),
            pltpu.VMEM((devices, pad_tiles, LANES), bf16),
            pltpu.VMEM((devices * pad_tiles + SUB, LANES), f32),
            pltpu.VMEM((-(-blocks // 8) * 8, entries), f32),
            pltpu.VMEM((devices * part_rows, 2 * entries), bf16),
            pltpu.VMEM((blocks, LANES, LANES), f32),
            pltpu.VMEM((blocks, LANES, LANES), f32),
            pltpu.VMEM((entries, LANES), f32),
            pltpu.VMEM((2, chunks, rows, keep), f32),
            pltpu.VMEM((2, devices, rows, keep), f32),
            pltpu.VMEM((2, rows, keep), f32),
            pltpu.VMEM((2, devices, rows, keep), f32),
            pltpu.VMEM((keep // 2, keep), f32),
            pltpu.VMEM((2, 1, keep), f32),
            pltpu.VMEM((2, 2, keep), f32),
            pltpu.VMEM((2, devices, 2, keep), f32),
            pltpu.VMEM((devices, part_rows // 2 + 1, LANES), i32),
            pltpu.VMEM((devices, part_rows // 2 + 1, LANES), i32),
            pltpu.SemaphoreType.DMA((9,)),
            pltpu.SemaphoreType.DMA((8,)),
            pltpu.SemaphoreType.DMA((8,)),
        ],
        compiler_params=pltpu.CompilerParams(
            collective_id=0, has_side_effects=True, vmem_limit_bytes=MAIN_VMEM - 512 * (-(-(own_tiles + blocks + 1) // SUB) * SUB)
        ),
    )(
        beta_start,
        tile_count,
        tile_cols,
        u_start.reshape(blocks, LANES),
        v_start.reshape(own_tiles, LANES),
        tiles,
        left_basis,
        right_basis,
    )
    return pl.pallas_call(
        functools.partial(place_kernel, own_tiles, blocks),
        out_shape=(
            jax.ShapeDtypeStruct((1, left_rows), f32),
            jax.ShapeDtypeStruct((1, right_rows), f32),
            jax.ShapeDtypeStruct((2,), f32),
        ),
        in_specs=[vmem],
        out_specs=(vmem, vmem, vmem),
        compiler_params=pltpu.CompilerParams(vmem_limit_bytes=1048576),
    )(packed)


def solution(mesh):
    placed = (
        P(AXES, None, None, None),
        P(AXES, None),
        P(AXES),
        P(AXES),
        P(AXES),
        P(),
        P(AXES, None),
        P(AXES, None),
    )
    return jax.shard_map(
        on_device,
        mesh=mesh,
        in_specs=placed,
        out_specs=(P(None, AXES), P(None, AXES), P()),
        check_vma=False,
    )
```

```python
import functools
import math

import jax
import jax.numpy as jnp
from jax import lax
from jax.experimental import pallas as pl
from jax.experimental.pallas import tpu as pltpu
from jax.sharding import PartitionSpec as P

AXES = ("blk", "plane")
LANES = 128
SUB = 8
ON_MXU = (2, 5, 7)
NT_DIMS = (((1,), (1,)), ((), ()))
MAIN_VMEM = 67043328
MESH = pl.DeviceIdType.MESH
UNROLL_DEVICES = 32


def far_first(blks, planes):
    masks = [(b, p) for b in range(blks) for p in range(planes) if b or p]
    weight = lambda m: m[0] // 2 + m[0] % 2 + m[1] // 2 + 0.3 * (m[1] % 2)
    return sorted(masks, key=weight, reverse=True)


def flips(index, size):
    steps = []
    bit = 1
    while bit < size:
        steps.append(bit * (1 - 2 * lax.rem(index // bit, 2)))
        bit *= 2
    values = []
    for mask in range(size):
        value = index
        for k, step in enumerate(steps):
            if mask >> k & 1:
                value = value + step
        values.append(value)
    return values


def steps_kernel(
    blks,
    planes,
    own_tiles,
    left_scale,
    right_scale,
    beta_hbm,
    count_hbm,
    cols_hbm,
    u_hbm,
    v_hbm,
    tiles_hbm,
    left_hbm,
    right_hbm,
    out_ref,
    beta_s,
    count_s,
    cols_s,
    cols_v,
    u_scr,
    v_scr,
    tiles,
    left,
    right,
    left_t,
    right_t,
    v_send,
    v_all,
    v_table,
    cols_rows,
    put_hot,
    shift_scr,
    p_scr,
    contrib,
    gram_send,
    gram_recv,
    gram_sum,
    gram_all,
    gram_scr,
    diagonal,
    dot_send,
    dot_recv,
    part_send,
    part_recv,
    copy_sem,
    send_sem,
    recv_sem,
):
    devices = blks * planes
    blocks, slots = cols_v.shape
    keep = left.shape[1]
    me_blk, me_plane = lax.axis_index("blk"), lax.axis_index("plane")
    me = me_blk * planes + me_plane
    chunks, rows = gram_send.shape[1:3]
    pad_tiles = v_send.shape[0]
    words = part_send.shape[1] - 1
    part_rows = 2 * words
    entries = contrib.shape[0]
    stride = entries // blocks
    two_power = blks & (blks - 1) == 0 and planes & (planes - 1) == 0
    unrolled = two_power and devices <= UNROLL_DEVICES
    if unrolled:
        blk_of, plane_of = flips(me_blk, blks), flips(me_plane, planes)
        order = far_first(blks, planes)

    def each_other(act):
        if unrolled:
            for b, p in order:
                act(blk_of[b] * planes + plane_of[p], (blk_of[b], plane_of[p]))
            return

        def body(step, carry):
            other = lax.rem(me + step, devices)
            act(other, (other // planes, lax.rem(other, planes)))
            return carry

        lax.fori_loop(1, devices, body, 0)

    owners = gram_all.shape[1]
    owner_blks = owners // planes
    first_owner = (blks - owner_blks) // 2
    owner = (me_blk >= first_owner) & (me_blk < first_owner + owner_blks)
    my_part = me - first_owner * planes

    barrier = pltpu.get_barrier_semaphore()
    each_other(
        lambda other, place: pl.semaphore_signal(
            barrier, inc=1, device_id=place, device_id_type=MESH
        )
    )

    pairs = (
        (v_hbm, v_scr),
        (cols_hbm, cols_v),
        (count_hbm, count_s),
        (cols_hbm, cols_s),
        (beta_hbm, beta_s),
        (u_hbm, u_scr),
        (left_hbm, left),
        (right_hbm, right),
        (tiles_hbm, tiles),
    )
    loads = [pltpu.make_async_copy(a, b, copy_sem.at[i]) for i, (a, b) in enumerate(pairs)]
    for load in loads:
        load.start()
    v_load, cols_load, count_load, index_load, beta_load, u_load, left_load, right_load, tiles_load = loads

    def send_one(phase, source, landing, place):
        pltpu.make_async_remote_copy(
            src_ref=source,
            dst_ref=landing,
            send_sem=send_sem.at[phase],
            recv_sem=recv_sem.at[phase],
            device_id=place,
            device_id_type=MESH,
        ).start()

    def send_all(phase, source, landing):
        each_other(lambda other, place: send_one(phase, source(other), landing.at[me], place))

    def wait_all(sem, phase, landing):
        most = landing.at[pl.ds(0, devices - 1)]
        pltpu.make_async_copy(most, most, sem.at[phase]).wait()

    eye = lax.broadcasted_iota(jnp.int32, (LANES, LANES), 0) == lax.broadcasted_iota(
        jnp.int32, (LANES, LANES), 1
    )

    half = keep // 2
    half_row = lax.broadcasted_iota(jnp.int32, (half, keep), 0)
    half_lane = lax.broadcasted_iota(jnp.int32, (half, keep), 1)

    def to_col(row):
        return jnp.sum(jnp.where(eye, row, 0.0), axis=1, keepdims=True)

    def to_row(col):
        return jnp.sum(jnp.where(eye, col, 0.0), axis=0, keepdims=True)

    def fold(block):
        return jnp.sum(block.reshape(LANES // SUB, SUB, LANES), axis=0)

    v_load.wait()
    rounded = v_scr[...]
    if pad_tiles > own_tiles:
        rounded = jnp.concatenate(
            [rounded, jnp.zeros((pad_tiles - own_tiles, LANES), jnp.float32)], axis=0
        )
    rounded = rounded.astype(jnp.bfloat16)
    v_send[...] = rounded
    v_all[me] = rounded
    v_table[devices * pad_tiles :, :] = jnp.zeros((SUB, LANES), jnp.float32)

    def start_gram(side, basis_t):
        whole = basis_t[...]
        high = whole.astype(jnp.bfloat16)
        rest = whole - high.astype(jnp.float32)
        mid = rest.astype(jnp.bfloat16)
        low = (rest - mid.astype(jnp.float32)).astype(jnp.bfloat16)

        def product(a, b):
            return lax.dot_general(a, b, NT_DIMS, preferred_element_type=jnp.float32)

        cross = product(high, mid) + product(high, low)
        gram = product(high, high) + (cross + cross.T + product(mid, mid))
        top, low = gram[0:half, :], pltpu.roll(gram[half:, :], half, 1)
        folded = jnp.where(half_lane >= half_row, top, low)
        for c in range(chunks):
            gram_send[side, c] = folded[c * rows : (c + 1) * rows, :]
        diagonal[side] = jnp.sum(
            jnp.where(half_lane == half_row + half, gram[half:, :], 0.0), axis=0, keepdims=True
        )
        gram_recv[side, me] = gram_send[side, lax.rem(my_part + owners, chunks)]

    def send_gram(side, phase):
        def send(part, place):
            send_one(
                phase,
                gram_send.at[side, lax.rem(part, chunks)],
                gram_recv.at[side, me],
                place,
            )

        if unrolled:
            near = flips(lax.rem(me_blk, owner_blks), owner_blks)
            for k in reversed(range(owner_blks)):
                for p in reversed(range(planes)):
                    part = near[k] * planes + plane_of[p]
                    place = (first_owner + near[k], plane_of[p])
                    if k == first_owner and p == 0:
                        pl.when(jnp.logical_not(owner))(functools.partial(send, part, place))
                    else:
                        send(part, place)
            return

        def body(step, carry):
            part = lax.rem(me + step, owners)
            place = (first_owner + part // planes, lax.rem(part, planes))
            pl.when(part != my_part)(functools.partial(send, part, place))
            return carry

        lax.fori_loop(0, owners, body, 0)

    def share_gram(side, phase):
        @pl.when(owner)
        def _():
            wait_all(recv_sem, phase, gram_recv.at[side])
            mine = jnp.sum(gram_recv[side], axis=0)
            gram_sum[side] = mine
            gram_all[side, jnp.clip(my_part, 0, owners - 1)] = mine
            each_other(
                lambda other, place: send_one(
                    phase + 1, gram_sum.at[side], gram_all.at[side, my_part], place
                )
            )

    def wait_owned(sem, phase, landing):
        for mine, size in ((owner, owners - 1), (jnp.logical_not(owner), owners)):
            if size:
                most = landing.at[pl.ds(0, size)]
                pl.when(mine)(pltpu.make_async_copy(most, most, sem.at[phase]).wait)

    def finish_gram(side, phase):
        wait_owned(recv_sem, phase + 1, gram_all.at[side])
        for c in range(chunks):
            gram_scr[c * rows : (c + 1) * rows, :] = gram_all[side, c]
        folded = gram_scr[...]
        strict = jnp.concatenate(
            [
                jnp.where(half_lane > half_row, folded, 0.0),
                pltpu.roll(jnp.where(half_lane < half_row, folded, 0.0), half, 1),
            ],
            axis=0,
        )
        main = jnp.sum(jnp.where(half_lane == half_row, folded, 0.0), axis=0, keepdims=True)
        return strict + strict.T + jnp.where(eye, main, 0.0)

    left_load.wait()
    for r in range(left.shape[0] // LANES):
        left_t[:, r * LANES : (r + 1) * LANES] = left[r * LANES : (r + 1) * LANES, :].T
    start_gram(0, left_t)

    pl.semaphore_wait(barrier, devices - 1)
    send_all(0, lambda other: v_send, v_all)
    send_gram(0, 1)

    cols_load.wait()
    count_load.wait()
    index_load.wait()
    beta_load.wait()
    u_load.wait()
    cols_rows[...] = jnp.full(cols_rows.shape, -1.0, jnp.float32)
    for r in range(blocks):
        row = cols_v[r : r + 1, :]
        alive = lax.broadcasted_iota(jnp.int32, (1, slots), 1) < count_s[r]
        cols_rows[r : r + 1, 0:slots] = jnp.where(alive, row, -1).astype(jnp.float32)
    lane = lax.broadcasted_iota(jnp.int32, (1, entries), 1)
    line = jnp.full((1, entries), -1.0, jnp.float32)
    for r in range(blocks):
        row = cols_rows[r : r + 1, :]
        if r:
            row = pltpu.roll(row, r * stride, 1)
        line = jnp.where((lane >= r * stride) & (lane < r * stride + slots), row, line)
    whole = line.astype(jnp.int32)
    put_row = jnp.where(whole < 0, -1, whole // own_tiles * part_rows + whole % own_tiles)
    hot = jnp.where(
        lax.broadcasted_iota(jnp.int32, (put_hot.shape[0], entries), 0) == put_row, 1.0, 0.0
    ).astype(jnp.bfloat16)
    put_hot[:, 0:entries] = hot
    put_hot[:, entries:] = hot
    contrib[...] = jnp.zeros_like(contrib)
    beta = beta_s[0]
    for r in range(blocks):
        shift_scr[r] = jnp.where(eye, -beta * u_scr[r : r + 1, :], 0.0)

    right_load.wait()
    for t in range(own_tiles):
        right_t[:, t * LANES : (t + 1) * LANES] = right[t * LANES : (t + 1) * LANES, :].T
    start_gram(1, right_t)
    tiles_load.wait()

    wait_all(recv_sem, 0, v_all)
    v_table[0 : devices * pad_tiles, :] = (
        v_all[...].reshape(devices * pad_tiles, LANES).astype(jnp.float32)
    )
    dots = jnp.zeros((SUB, LANES), jnp.float32)
    square = jnp.zeros((SUB, LANES), jnp.float32)
    for r in range(blocks):
        if r == blocks - 1:
            share_gram(0, 1)
        total = shift_scr[r]
        for s in range(slots):
            col = cols_s[r, s]
            if pad_tiles != own_tiles:
                col = col // own_tiles * pad_tiles + lax.rem(col, own_tiles)
            col = jnp.where(s < count_s[r], col, devices * pad_tiles)
            total = total + tiles[r, s].astype(jnp.float32) * v_table[pl.ds(col, 1), :]
        p_col = jnp.broadcast_to(jnp.sum(total, axis=1, keepdims=True), (LANES, LANES))
        p_scr[r] = p_col
        dots = dots + fold(left[r * LANES : (r + 1) * LANES, :] * p_col)
        square = square + fold(p_col * p_col)

    def start_dots(side, dots, square):
        lane = lax.broadcasted_iota(jnp.int32, (1, keep), 1)
        both = jnp.concatenate([dots, jnp.where(lane >= half, diagonal[side], square)], axis=0)
        dot_send[side] = both
        dot_recv[side, me] = both
        send_all(3 + side, lambda other: dot_send.at[side], dot_recv.at[side])

    def finish_dots(side, phase):
        gram = finish_gram(side, phase)
        wait_all(recv_sem, 3 + side, dot_recv.at[side])
        both = jnp.sum(dot_recv[side], axis=0)
        first, square = both[0:1, :], both[1:2, 0:1]
        lane = lax.broadcasted_iota(jnp.int32, (1, keep), 1)
        gram = gram + jnp.where(eye & (lane >= half), both[1:2, :], 0.0)
        twice = jnp.where(eye, 2.0, 0.0) - gram
        coef = jnp.sum(twice * first, axis=1, keepdims=True)
        coef_row = to_row(coef)
        spread = jnp.sum(gram * coef, axis=0, keepdims=True)
        change = jnp.sum(coef_row * (spread - 2.0 * first), axis=1, keepdims=True)
        return coef, coef_row, jnp.sqrt(square + change + 1e-06)

    start_dots(
        0, jnp.sum(dots, axis=0, keepdims=True), jnp.sum(square, axis=0, keepdims=True)
    )
    send_gram(1, 6)

    coef, coef_row, alpha = finish_dots(0, 1)
    inverse = 1.0 / alpha

    for r in range(blocks):
        fix = jnp.sum(left[r * LANES : (r + 1) * LANES, :] * coef_row, axis=1, keepdims=True)
        p_scr[r] = (p_scr[r] - fix) * inverse

    spot = lax.broadcasted_iota(jnp.int32, (SUB, LANES), 0)
    for r in range(blocks):
        rounded = p_scr[r].astype(jnp.bfloat16)
        col = rounded.astype(jnp.float32)
        row = jnp.broadcast_to(to_row(col), (2 * SUB, LANES)).astype(jnp.bfloat16)
        for g in range(0, slots, SUB):
            lines = jnp.zeros((SUB, LANES), jnp.float32)
            for s in range(g, min(g + SUB, slots)):
                if s % SUB in ON_MXU:
                    line = jnp.dot(row, tiles[r, s], preferred_element_type=jnp.float32)[0:SUB, :]
                else:
                    line = jnp.sum(fold(tiles[r, s].astype(jnp.float32) * col), axis=0, keepdims=True)
                lines = jnp.where(spot == s - g, line, lines)
            contrib[r * stride + g : r * stride + g + SUB, :] = lines
    whole = contrib[...]
    high = whole.astype(jnp.bfloat16)
    low = (whole - high.astype(jnp.float32)).astype(jnp.bfloat16)
    spread = jnp.dot(
        put_hot[...], jnp.concatenate([high, low], axis=0), preferred_element_type=jnp.float32
    )
    parts = spread.reshape(devices, part_rows, LANES)
    top = jnp.maximum(jnp.max(jnp.abs(parts), axis=1, keepdims=True), 1e-30)
    power = jnp.floor(jnp.log2(top)) - 14.0
    whole = jnp.minimum(jnp.round(parts * jnp.exp2(-power)), 32767.0).astype(jnp.int32)
    part_send[:, 0:words, :] = lax.shift_left(whole[:, 0:words, :], 16) | (
        whole[:, words:, :] & 0xFFFF
    )
    part_send[:, words:, :] = power.astype(jnp.int32)
    part_recv[me] = part_send[me]
    send_all(5, lambda other: part_send.at[other], part_recv)
    for r in range(blocks):
        out_ref[own_tiles + r : own_tiles + r + 1, :] = to_row(p_scr[r]) * left_scale
    wait_all(recv_sem, 5, part_recv)
    share_gram(1, 6)
    unit = jnp.exp2(part_recv[:, words:, :].astype(jnp.float32))
    word = part_recv[:, 0:words, :]
    halves = (lax.shift_right_arithmetic(word, 16), lax.shift_right_arithmetic(lax.shift_left(word, 16), 16))
    own = jnp.concatenate(
        [jnp.sum(half.astype(jnp.float32) * unit, axis=0) for half in halves], axis=0
    )
    r_vec = own[0:own_tiles, :] - alpha * v_scr[...]

    total = jnp.zeros((keep, LANES), jnp.float32)
    for t in range(own_tiles):
        total = total + right_t[:, t * LANES : (t + 1) * LANES] * r_vec[t : t + 1, :]
    dots = to_row(jnp.sum(total, axis=1, keepdims=True))
    square = jnp.sum(r_vec * r_vec, keepdims=True)
    start_dots(1, dots, jnp.broadcast_to(square, (1, LANES)))
    coef, coef_row, beta_new = finish_dots(1, 6)
    place = lax.broadcasted_iota(jnp.int32, (1, LANES), 1)
    out_ref[own_tiles + blocks : own_tiles + blocks + 1, :] = jnp.where(
        place == 0, alpha, beta_new
    )
    inverse = right_scale / beta_new
    for t in range(own_tiles):
        fix = jnp.sum(right_t[:, t * LANES : (t + 1) * LANES] * coef, axis=0, keepdims=True)
        out_ref[t : t + 1, :] = (r_vec[t : t + 1, :] - fix) * inverse

    wait_all(send_sem, 0, v_all)
    for phase, side in ((1, 0), (6, 1)):
        wait_owned(send_sem, phase, gram_all.at[side])
        pl.when(owner)(functools.partial(wait_all, send_sem, phase + 1, gram_recv.at[side]))
    wait_all(send_sem, 3, dot_recv.at[0])
    wait_all(send_sem, 4, dot_recv.at[1])
    wait_all(send_sem, 5, part_recv)


def place_kernel(own_tiles, blocks, packed, out_left, out_right, out_coef):
    for r in range(blocks):
        out_left[:, r * LANES : (r + 1) * LANES] = packed[own_tiles + r : own_tiles + r + 1, :]
    for t in range(own_tiles):
        out_right[:, t * LANES : (t + 1) * LANES] = packed[t : t + 1, :]
    out_coef[...] = packed[own_tiles + blocks, 0:2]


def on_device(tiles, tile_cols, tile_count, u_start, v_start, beta_start, left_basis, right_basis):
    blks, planes = lax.axis_size("blk"), lax.axis_size("plane")
    devices = blks * planes
    blocks, slots = tile_cols.shape
    own_tiles = v_start.shape[0] // LANES
    left_rows, keep = left_basis.shape
    right_rows = right_basis.shape[0]
    pad_tiles = -(-own_tiles // 16) * 16
    part_rows = -(-own_tiles // 16) * 16
    owners = (blks // 2 if blks % 4 == 0 else blks) * planes
    rows = max(2, keep // 2 // owners)
    chunks = keep // 2 // rows
    stride = -(-slots // 8) * 8
    while (blocks * stride) % LANES:
        stride += 8
    entries = blocks * stride
    f32, bf16, i32 = jnp.float32, jnp.bfloat16, jnp.int32
    vmem = pl.BlockSpec(memory_space=pltpu.VMEM)
    hbm = pl.BlockSpec(memory_space=pl.ANY)
    packed = pl.pallas_call(
        functools.partial(
            steps_kernel,
            blks,
            planes,
            own_tiles,
            math.sqrt(left_rows * devices),
            math.sqrt(right_rows * devices),
        ),
        out_shape=pltpu.VMEM((own_tiles + blocks + 1, LANES), f32),
        in_specs=[hbm] * 8,
        out_specs=vmem,
        scratch_shapes=[
            pltpu.SMEM((1,), f32),
            pltpu.SMEM((blocks,), i32),
            pltpu.SMEM((blocks, slots), i32),
            pltpu.VMEM((blocks, slots), i32),
            pltpu.VMEM((blocks, LANES), f32),
            pltpu.VMEM((own_tiles, LANES), f32),
            pltpu.VMEM(tiles.shape, bf16),
            pltpu.VMEM(left_basis.shape, f32),
            pltpu.VMEM(right_basis.shape, f32),
            pltpu.VMEM((keep, left_rows), f32),
            pltpu.VMEM((keep, right_rows), f32),
            pltpu.VMEM((pad_tiles, LANES), bf16),
            pltpu.VMEM((devices, pad_tiles, LANES), bf16),
            pltpu.VMEM((devices * pad_tiles + SUB, LANES), f32),
            pltpu.VMEM((-(-blocks // 8) * 8, entries), f32),
            pltpu.VMEM((devices * part_rows, 2 * entries), bf16),
            pltpu.VMEM((blocks, LANES, LANES), f32),
            pltpu.VMEM((blocks, LANES, LANES), f32),
            pltpu.VMEM((entries, LANES), f32),
            pltpu.VMEM((2, chunks, rows, keep), f32),
            pltpu.VMEM((2, devices, rows, keep), f32),
            pltpu.VMEM((2, rows, keep), f32),
            pltpu.VMEM((2, owners, rows, keep), f32),
            pltpu.VMEM((keep // 2, keep), f32),
            pltpu.VMEM((2, 1, keep), f32),
            pltpu.VMEM((2, 2, keep), f32),
            pltpu.VMEM((2, devices, 2, keep), f32),
            pltpu.VMEM((devices, part_rows // 2 + 1, LANES), i32),
            pltpu.VMEM((devices, part_rows // 2 + 1, LANES), i32),
            pltpu.SemaphoreType.DMA((9,)),
            pltpu.SemaphoreType.DMA((8,)),
            pltpu.SemaphoreType.DMA((8,)),
        ],
        compiler_params=pltpu.CompilerParams(
            collective_id=0, has_side_effects=True, vmem_limit_bytes=MAIN_VMEM - 512 * (-(-(own_tiles + blocks + 1) // SUB) * SUB)
        ),
    )(
        beta_start,
        tile_count,
        tile_cols,
        u_start.reshape(blocks, LANES),
        v_start.reshape(own_tiles, LANES),
        tiles,
        left_basis,
        right_basis,
    )
    return pl.pallas_call(
        functools.partial(place_kernel, own_tiles, blocks),
        out_shape=(
            jax.ShapeDtypeStruct((1, left_rows), f32),
            jax.ShapeDtypeStruct((1, right_rows), f32),
            jax.ShapeDtypeStruct((2,), f32),
        ),
        in_specs=[vmem],
        out_specs=(vmem, vmem, vmem),
        compiler_params=pltpu.CompilerParams(vmem_limit_bytes=1048576),
    )(packed)


def solution(mesh):
    placed = (
        P(AXES, None, None, None),
        P(AXES, None),
        P(AXES),
        P(AXES),
        P(AXES),
        P(),
        P(AXES, None),
        P(AXES, None),
    )
    return jax.shard_map(
        on_device,
        mesh=mesh,
        in_specs=placed,
        out_specs=(P(None, AXES), P(None, AXES), P()),
        check_vma=False,
    )
```

```python
import functools
import math

import jax
import jax.numpy as jnp
from jax import lax
from jax.experimental import pallas as pl
from jax.experimental.pallas import tpu as pltpu
from jax.sharding import PartitionSpec as P

AXES = ("blk", "plane")
LANES = 128
SUB = 8
ON_MXU = (0, 1, 2)
NT_DIMS = (((1,), (1,)), ((), ()))
MAIN_VMEM = 67043328
MESH = pl.DeviceIdType.MESH
RECV = (0, 1, 2, 3, 3, 0, 4, 2)
UNROLL_DEVICES = 32


def far_first(blks, planes):
    masks = [(b, p) for b in range(blks) for p in range(planes) if b or p]
    weight = lambda m: 0.6 * (m[0] // 2) + m[0] % 2 + m[1] // 2 - 0.3 * (m[1] % 2)
    return sorted(masks, key=weight, reverse=True)


def flips(index, size):
    steps = []
    bit = 1
    while bit < size:
        steps.append(bit * (1 - 2 * lax.rem(index // bit, 2)))
        bit *= 2
    values = []
    for mask in range(size):
        value = index
        for k, step in enumerate(steps):
            if mask >> k & 1:
                value = value + step
        values.append(value)
    return values


def steps_kernel(
    blks,
    planes,
    own_tiles,
    left_scale,
    right_scale,
    beta_hbm,
    count_hbm,
    cols_hbm,
    u_hbm,
    v_hbm,
    tiles_hbm,
    left_hbm,
    right_hbm,
    out_ref,
    beta_s,
    count_s,
    cols_s,
    cols_v,
    u_scr,
    v_scr,
    tiles,
    left,
    right,
    left_t,
    right_t,
    v_send,
    v_all,
    v_table,
    cols_rows,
    put_hot,
    shift_scr,
    p_scr,
    contrib,
    gram_send,
    gram_recv,
    gram_sum,
    gram_all,
    gram_scr,
    diagonal,
    dot_send,
    dot_recv,
    part_send,
    part_recv,
    sent,
    copy_sem,
    send_sem,
    recv_sem,
):
    devices = blks * planes
    blocks, slots = cols_v.shape
    keep = left.shape[1]
    me_blk, me_plane = lax.axis_index("blk"), lax.axis_index("plane")
    me = me_blk * planes + me_plane
    chunks, rows = gram_send.shape[1:3]
    pad_tiles = v_send.shape[0]
    words = part_send.shape[1] - 1
    part_rows = 2 * words
    entries = contrib.shape[0]
    stride = entries // blocks
    two_power = blks & (blks - 1) == 0 and planes & (planes - 1) == 0
    unrolled = two_power and devices <= UNROLL_DEVICES
    if unrolled:
        blk_of, plane_of = flips(me_blk, blks), flips(me_plane, planes)
        order = far_first(blks, planes)

    def each_other(act):
        if unrolled:
            for b, p in order:
                act(blk_of[b] * planes + plane_of[p], (blk_of[b], plane_of[p]))
            return

        def body(step, carry):
            other = lax.rem(me + step, devices)
            act(other, (other // planes, lax.rem(other, planes)))
            return carry

        lax.fori_loop(1, devices, body, 0)

    owners = gram_all.shape[1]
    owner_blks = owners // planes
    first_owner = (blks - owner_blks) // 2
    owner = (me_blk >= first_owner) & (me_blk < first_owner + owner_blks)
    my_part = me - first_owner * planes

    barrier = pltpu.get_barrier_semaphore()
    each_other(
        lambda other, place: pl.semaphore_signal(
            barrier, inc=1, device_id=place, device_id_type=MESH
        )
    )

    pairs = (
        (v_hbm, v_scr),
        (cols_hbm, cols_v),
        (count_hbm, count_s),
        (cols_hbm, cols_s),
        (beta_hbm, beta_s),
        (u_hbm, u_scr),
        (left_hbm, left),
        (right_hbm, right),
        (tiles_hbm, tiles),
    )
    loads = [pltpu.make_async_copy(a, b, copy_sem.at[i]) for i, (a, b) in enumerate(pairs)]
    for load in loads:
        load.start()
    v_load, cols_load, count_load, index_load, beta_load, u_load, left_load, right_load, tiles_load = loads

    def send_one(phase, source, landing, place):
        pltpu.make_async_remote_copy(
            src_ref=source,
            dst_ref=landing,
            send_sem=send_sem.at[0],
            recv_sem=recv_sem.at[RECV[phase]],
            device_id=place,
            device_id_type=MESH,
        ).start()

    def send_all(phase, source, landing):
        each_other(lambda other, place: send_one(phase, source(other), landing.at[me], place))

    def wait_all(phase, landing):
        most = landing.at[pl.ds(0, devices - 1)]
        pltpu.make_async_copy(most, most, recv_sem.at[RECV[phase]]).wait()

    eye = lax.broadcasted_iota(jnp.int32, (LANES, LANES), 0) == lax.broadcasted_iota(
        jnp.int32, (LANES, LANES), 1
    )

    half = keep // 2
    half_row = lax.broadcasted_iota(jnp.int32, (half, keep), 0)
    half_lane = lax.broadcasted_iota(jnp.int32, (half, keep), 1)

    def to_col(row):
        return jnp.sum(jnp.where(eye, row, 0.0), axis=1, keepdims=True)

    def to_row(col):
        return jnp.sum(jnp.where(eye, col, 0.0), axis=0, keepdims=True)

    def fold(block):
        return jnp.sum(block.reshape(LANES // SUB, SUB, LANES), axis=0)

    v_load.wait()
    rounded = v_scr[...]
    if pad_tiles > own_tiles:
        rounded = jnp.concatenate(
            [rounded, jnp.zeros((pad_tiles - own_tiles, LANES), jnp.float32)], axis=0
        )
    rounded = rounded.astype(jnp.bfloat16)
    v_send[...] = rounded
    v_all[me] = rounded
    v_table[devices * pad_tiles :, :] = jnp.zeros((SUB, LANES), jnp.float32)

    def start_gram(side, basis_t):
        whole = basis_t[...]
        high = whole.astype(jnp.bfloat16)
        rest = whole - high.astype(jnp.float32)
        mid = rest.astype(jnp.bfloat16)
        low = (rest - mid.astype(jnp.float32)).astype(jnp.bfloat16)

        def product(a, b):
            return lax.dot_general(a, b, NT_DIMS, preferred_element_type=jnp.float32)

        cross = product(high, mid) + product(high, low)
        gram = product(high, high) + (cross + cross.T + product(mid, mid))
        top, low = gram[0:half, :], pltpu.roll(gram[half:, :], half, 1)
        folded = jnp.where(half_lane >= half_row, top, low)
        for c in range(chunks):
            gram_send[side, c] = folded[c * rows : (c + 1) * rows, :]
        diagonal[side] = jnp.sum(
            jnp.where(half_lane == half_row + half, gram[half:, :], 0.0), axis=0, keepdims=True
        )
        gram_recv[side, me] = gram_send[side, lax.rem(my_part + owners, chunks)]

    def send_gram(side, phase):
        def send(part, place):
            send_one(
                phase,
                gram_send.at[side, lax.rem(part, chunks)],
                gram_recv.at[side, me],
                place,
            )

        if unrolled:
            near = flips(lax.rem(me_blk, owner_blks), owner_blks)
            for k in reversed(range(owner_blks)):
                for p in reversed(range(planes)):
                    part = near[k] * planes + plane_of[p]
                    place = (first_owner + near[k], plane_of[p])
                    if k == first_owner and p == 0:
                        pl.when(jnp.logical_not(owner))(functools.partial(send, part, place))
                    else:
                        send(part, place)
            return

        def body(step, carry):
            part = lax.rem(me + step, owners)
            place = (first_owner + part // planes, lax.rem(part, planes))
            pl.when(part != my_part)(functools.partial(send, part, place))
            return carry

        lax.fori_loop(0, owners, body, 0)

    def share_gram(side, phase):
        @pl.when(owner)
        def _():
            wait_all(phase, gram_recv.at[side])
            mine = jnp.sum(gram_recv[side], axis=0)
            gram_sum[side] = mine
            gram_all[side, jnp.clip(my_part, 0, owners - 1)] = mine
            each_other(
                lambda other, place: send_one(
                    phase + 1, gram_sum.at[side], gram_all.at[side, my_part], place
                )
            )

    def wait_owned(phase, landing):
        for mine, size in ((owner, owners - 1), (jnp.logical_not(owner), owners)):
            if size:
                most = landing.at[pl.ds(0, size)]
                pl.when(mine)(pltpu.make_async_copy(most, most, recv_sem.at[RECV[phase]]).wait)

    def finish_gram(side, phase):
        wait_owned(phase + 1, gram_all.at[side])
        for c in range(chunks):
            gram_scr[c * rows : (c + 1) * rows, :] = gram_all[side, c]
        folded = gram_scr[...]
        strict = jnp.concatenate(
            [
                jnp.where(half_lane > half_row, folded, 0.0),
                pltpu.roll(jnp.where(half_lane < half_row, folded, 0.0), half, 1),
            ],
            axis=0,
        )
        main = jnp.sum(jnp.where(half_lane == half_row, folded, 0.0), axis=0, keepdims=True)
        return strict + strict.T + jnp.where(eye, main, 0.0)

    left_load.wait()
    for r in range(left.shape[0] // LANES):
        left_t[:, r * LANES : (r + 1) * LANES] = left[r * LANES : (r + 1) * LANES, :].T
    start_gram(0, left_t)

    pl.semaphore_wait(barrier, devices - 1)
    send_all(0, lambda other: v_send, v_all)
    send_gram(0, 1)

    cols_load.wait()
    count_load.wait()
    index_load.wait()
    beta_load.wait()
    u_load.wait()
    cols_rows[...] = jnp.full(cols_rows.shape, -1.0, jnp.float32)
    for r in range(blocks):
        row = cols_v[r : r + 1, :]
        alive = lax.broadcasted_iota(jnp.int32, (1, slots), 1) < count_s[r]
        cols_rows[r : r + 1, 0:slots] = jnp.where(alive, row, -1).astype(jnp.float32)
    lane = lax.broadcasted_iota(jnp.int32, (1, entries), 1)
    line = jnp.full((1, entries), -1.0, jnp.float32)
    for r in range(blocks):
        row = cols_rows[r : r + 1, :]
        if r:
            row = pltpu.roll(row, r * stride, 1)
        line = jnp.where((lane >= r * stride) & (lane < r * stride + slots), row, line)
    whole = line.astype(jnp.int32)
    put_row = jnp.where(whole < 0, -1, whole // own_tiles * part_rows + whole % own_tiles)
    hot = jnp.where(
        lax.broadcasted_iota(jnp.int32, (put_hot.shape[0], entries), 0) == put_row, 1.0, 0.0
    ).astype(jnp.bfloat16)
    put_hot[:, 0:entries] = hot
    put_hot[:, entries:] = hot
    contrib[...] = jnp.zeros_like(contrib)
    beta = beta_s[0]
    for r in range(blocks):
        shift_scr[r] = jnp.where(eye, -beta * u_scr[r : r + 1, :], 0.0)

    right_load.wait()
    for t in range(own_tiles):
        right_t[:, t * LANES : (t + 1) * LANES] = right[t * LANES : (t + 1) * LANES, :].T
    start_gram(1, right_t)
    tiles_load.wait()

    wait_all(0, v_all)
    v_table[0 : devices * pad_tiles, :] = (
        v_all[...].reshape(devices * pad_tiles, LANES).astype(jnp.float32)
    )
    for r in range(blocks):
        if r == blocks - 1:
            share_gram(0, 1)
        total = shift_scr[r]
        for s in range(slots):
            col = cols_s[r, s]
            if pad_tiles != own_tiles:
                col = col // own_tiles * pad_tiles + lax.rem(col, own_tiles)
            col = jnp.where(s < count_s[r], col, devices * pad_tiles)
            total = total + tiles[r, s].astype(jnp.float32) * v_table[pl.ds(col, 1), :]
        p_scr[r] = total
    dots = jnp.zeros((SUB, LANES), jnp.float32)
    square = jnp.zeros((SUB, LANES), jnp.float32)
    for r in range(blocks):
        p_col = jnp.broadcast_to(jnp.sum(p_scr[r], axis=1, keepdims=True), (LANES, LANES))
        p_scr[r] = p_col
        dots = dots + fold(left[r * LANES : (r + 1) * LANES, :] * p_col)
        square = square + fold(p_col * p_col)

    def start_dots(side, dots, square):
        lane = lax.broadcasted_iota(jnp.int32, (1, keep), 1)
        both = jnp.concatenate([dots, jnp.where(lane >= half, diagonal[side], square)], axis=0)
        dot_send[side] = both
        dot_recv[side, me] = both
        send_all(3 + side, lambda other: dot_send.at[side], dot_recv.at[side])

    def finish_dots(side, phase):
        gram = finish_gram(side, phase)
        wait_all(3 + side, dot_recv.at[side])
        both = jnp.sum(dot_recv[side], axis=0)
        first, square = both[0:1, :], both[1:2, 0:1]
        lane = lax.broadcasted_iota(jnp.int32, (1, keep), 1)
        gram = gram + jnp.where(eye & (lane >= half), both[1:2, :], 0.0)
        twice = jnp.where(eye, 2.0, 0.0) - gram
        coef = jnp.sum(twice * first, axis=1, keepdims=True)
        coef_row = to_row(coef)
        spread = jnp.sum(gram * coef, axis=0, keepdims=True)
        change = jnp.sum(coef_row * (spread - 2.0 * first), axis=1, keepdims=True)
        return coef, coef_row, square + change + 1e-06

    start_dots(
        0, jnp.sum(dots, axis=0, keepdims=True), jnp.sum(square, axis=0, keepdims=True)
    )
    send_gram(1, 6)

    coef, coef_row, total = finish_dots(0, 1)
    inverse, alpha = lax.rsqrt(total), jnp.sqrt(total)

    for r in range(blocks):
        fix = jnp.sum(left[r * LANES : (r + 1) * LANES, :] * coef_row, axis=1, keepdims=True)
        p_scr[r] = (p_scr[r] - fix) * inverse

    spot = lax.broadcasted_iota(jnp.int32, (SUB, LANES), 0)
    for r in range(blocks):
        rounded = p_scr[r].astype(jnp.bfloat16)
        col = rounded.astype(jnp.float32)
        row = jnp.broadcast_to(to_row(col), (2 * SUB, LANES)).astype(jnp.bfloat16)
        for g in range(0, slots, SUB):
            lines = jnp.zeros((SUB, LANES), jnp.float32)
            for s in range(g, min(g + SUB, slots)):
                if s % SUB in ON_MXU:
                    line = jnp.dot(row, tiles[r, s], preferred_element_type=jnp.float32)[0:SUB, :]
                else:
                    line = jnp.sum(fold(tiles[r, s].astype(jnp.float32) * col), axis=0, keepdims=True)
                lines = jnp.where(spot == s - g, line, lines)
            contrib[r * stride + g : r * stride + g + SUB, :] = lines
    whole = contrib[...]
    high = whole.astype(jnp.bfloat16)
    low = (whole - high.astype(jnp.float32)).astype(jnp.bfloat16)
    spread = jnp.dot(
        put_hot[...], jnp.concatenate([high, low], axis=0), preferred_element_type=jnp.float32
    )
    parts = spread.reshape(devices, part_rows, LANES)
    top = jnp.maximum(jnp.max(jnp.abs(parts), axis=1, keepdims=True), 1e-30)
    power = jnp.floor(jnp.log2(top)) - 14.0
    whole = jnp.minimum(jnp.round(parts * jnp.exp2(-power)), 32767.0).astype(jnp.int32)
    part_send[:, 0:words, :] = lax.shift_left(whole[:, 0:words, :], 16) | (
        whole[:, words:, :] & 0xFFFF
    )
    part_send[:, words:, :] = power.astype(jnp.int32)
    part_recv[me] = part_send[me]
    send_all(5, lambda other: part_send.at[other], part_recv)
    for r in range(blocks):
        out_ref[own_tiles + r : own_tiles + r + 1, :] = to_row(p_scr[r]) * left_scale
    wait_all(5, part_recv)
    share_gram(1, 6)
    unit = jnp.exp2(part_recv[:, words:, :].astype(jnp.float32))
    word = part_recv[:, 0:words, :]
    halves = (lax.shift_right_arithmetic(word, 16), lax.shift_right_arithmetic(lax.shift_left(word, 16), 16))
    own = jnp.concatenate(
        [jnp.sum(half.astype(jnp.float32) * unit, axis=0) for half in halves], axis=0
    )
    r_vec = own[0:own_tiles, :] - alpha * v_scr[...]

    total = jnp.zeros((keep, LANES), jnp.float32)
    for t in range(own_tiles):
        total = total + right_t[:, t * LANES : (t + 1) * LANES] * r_vec[t : t + 1, :]
    dots = to_row(jnp.sum(total, axis=1, keepdims=True))
    square = jnp.sum(r_vec * r_vec, keepdims=True)
    start_dots(1, dots, jnp.broadcast_to(square, (1, LANES)))
    coef, coef_row, total = finish_dots(1, 6)
    beta_new = jnp.sqrt(total)
    place = lax.broadcasted_iota(jnp.int32, (1, LANES), 1)
    out_ref[own_tiles + blocks : own_tiles + blocks + 1, :] = jnp.where(
        place == 0, alpha, beta_new
    )
    inverse = right_scale * lax.rsqrt(total)
    for t in range(own_tiles):
        fix = jnp.sum(right_t[:, t * LANES : (t + 1) * LANES] * coef, axis=0, keepdims=True)
        out_ref[t : t + 1, :] = (r_vec[t : t + 1, :] - fix) * inverse

    each = v_send.shape[0] // 2 + 2 * dot_send.shape[1] + part_send.shape[1]
    grams = 2 * rows
    for mine, size in (
        (owner, (devices - 1) * (each + grams) + (owners - 1) * grams),
        (jnp.logical_not(owner), (devices - 1) * each + owners * grams),
    ):
        most = sent.at[pl.ds(0, size)]
        pl.when(mine)(pltpu.make_async_copy(most, most, send_sem.at[0]).wait)


def place_kernel(own_tiles, blocks, packed, out_left, out_right, out_coef):
    for r in range(blocks):
        out_left[:, r * LANES : (r + 1) * LANES] = packed[own_tiles + r : own_tiles + r + 1, :]
    for t in range(own_tiles):
        out_right[:, t * LANES : (t + 1) * LANES] = packed[t : t + 1, :]
    out_coef[...] = packed[own_tiles + blocks, 0:2]


def on_device(tiles, tile_cols, tile_count, u_start, v_start, beta_start, left_basis, right_basis):
    blks, planes = lax.axis_size("blk"), lax.axis_size("plane")
    devices = blks * planes
    blocks, slots = tile_cols.shape
    own_tiles = v_start.shape[0] // LANES
    left_rows, keep = left_basis.shape
    right_rows = right_basis.shape[0]
    pad_tiles = -(-own_tiles // 16) * 16
    part_rows = -(-own_tiles // 16) * 16
    owners = (blks // 2 if blks % 4 == 0 else blks) * planes
    rows = max(2, keep // 2 // owners)
    chunks = keep // 2 // rows
    stride = -(-slots // 8) * 8
    while (blocks * stride) % LANES:
        stride += 8
    entries = blocks * stride
    sent_rows = (devices - 1) * (pad_tiles // 2 + 4 + part_rows // 2 + 1 + 2 * rows)
    sent_rows += owners * 2 * rows
    f32, bf16, i32 = jnp.float32, jnp.bfloat16, jnp.int32
    vmem = pl.BlockSpec(memory_space=pltpu.VMEM)
    hbm = pl.BlockSpec(memory_space=pl.ANY)
    packed = pl.pallas_call(
        functools.partial(
            steps_kernel,
            blks,
            planes,
            own_tiles,
            math.sqrt(left_rows * devices),
            math.sqrt(right_rows * devices),
        ),
        out_shape=pltpu.VMEM((own_tiles + blocks + 1, LANES), f32),
        in_specs=[hbm] * 8,
        out_specs=vmem,
        scratch_shapes=[
            pltpu.SMEM((1,), f32),
            pltpu.SMEM((blocks,), i32),
            pltpu.SMEM((blocks, slots), i32),
            pltpu.VMEM((blocks, slots), i32),
            pltpu.VMEM((blocks, LANES), f32),
            pltpu.VMEM((own_tiles, LANES), f32),
            pltpu.VMEM(tiles.shape, bf16),
            pltpu.VMEM(left_basis.shape, f32),
            pltpu.VMEM(right_basis.shape, f32),
            pltpu.VMEM((keep, left_rows), f32),
            pltpu.VMEM((keep, right_rows), f32),
            pltpu.VMEM((pad_tiles, LANES), bf16),
            pltpu.VMEM((devices, pad_tiles, LANES), bf16),
            pltpu.VMEM((devices * pad_tiles + SUB, LANES), f32),
            pltpu.VMEM((-(-blocks // 8) * 8, entries), f32),
            pltpu.VMEM((devices * part_rows, 2 * entries), bf16),
            pltpu.VMEM((blocks, LANES, LANES), f32),
            pltpu.VMEM((blocks, LANES, LANES), f32),
            pltpu.VMEM((entries, LANES), f32),
            pltpu.VMEM((2, chunks, rows, keep), f32),
            pltpu.VMEM((2, devices, rows, keep), f32),
            pltpu.VMEM((2, rows, keep), f32),
            pltpu.VMEM((2, owners, rows, keep), f32),
            pltpu.VMEM((keep // 2, keep), f32),
            pltpu.VMEM((2, 1, keep), f32),
            pltpu.VMEM((2, 2, keep), f32),
            pltpu.VMEM((2, devices, 2, keep), f32),
            pltpu.VMEM((devices, part_rows // 2 + 1, LANES), i32),
            pltpu.VMEM((devices, part_rows // 2 + 1, LANES), i32),
            pltpu.VMEM((sent_rows, LANES), f32),
            pltpu.SemaphoreType.DMA((9,)),
            pltpu.SemaphoreType.DMA((1,)),
            pltpu.SemaphoreType.DMA((5,)),
        ],
        compiler_params=pltpu.CompilerParams(
            collective_id=0, has_side_effects=True, vmem_limit_bytes=MAIN_VMEM - 512 * (-(-(own_tiles + blocks + 1) // SUB) * SUB)
        ),
    )(
        beta_start,
        tile_count,
        tile_cols,
        u_start.reshape(blocks, LANES),
        v_start.reshape(own_tiles, LANES),
        tiles,
        left_basis,
        right_basis,
    )
    return pl.pallas_call(
        functools.partial(place_kernel, own_tiles, blocks),
        out_shape=(
            jax.ShapeDtypeStruct((1, left_rows), f32),
            jax.ShapeDtypeStruct((1, right_rows), f32),
            jax.ShapeDtypeStruct((2,), f32),
        ),
        in_specs=[vmem],
        out_specs=(vmem, vmem, vmem),
        compiler_params=pltpu.CompilerParams(vmem_limit_bytes=1048576),
    )(packed)


def solution(mesh):
    placed = (
        P(AXES, None, None, None),
        P(AXES, None),
        P(AXES),
        P(AXES),
        P(AXES),
        P(),
        P(AXES, None),
        P(AXES, None),
    )
    return jax.shard_map(
        on_device,
        mesh=mesh,
        in_specs=placed,
        out_specs=(P(None, AXES), P(None, AXES), P()),
        check_vma=False,
    )
```

```python
import functools
import math

import jax
import jax.numpy as jnp
from jax import lax
from jax.experimental import pallas as pl
from jax.experimental.pallas import tpu as pltpu
from jax.sharding import PartitionSpec as P

AXES = ("blk", "plane")
LANES = 128
SUB = 8
ON_MXU = (0, 1, 2)
NT_DIMS = (((1,), (1,)), ((), ()))
MAIN_VMEM = 67043328
MESH = pl.DeviceIdType.MESH
RECV = (0, 1, 2, 3, 3, 0, 4, 2)
UNROLL_DEVICES = 32


def far_first(blks, planes):
    masks = [(b, p) for b in range(blks) for p in range(planes) if b or p]
    weight = lambda m: 0.6 * (m[0] // 2) + m[0] % 2 + m[1] // 2 - 0.3 * (m[1] % 2)
    return sorted(masks, key=weight, reverse=True)


def flips(index, size):
    steps = []
    bit = 1
    while bit < size:
        steps.append(bit * (1 - 2 * lax.rem(index // bit, 2)))
        bit *= 2
    values = []
    for mask in range(size):
        value = index
        for k, step in enumerate(steps):
            if mask >> k & 1:
                value = value + step
        values.append(value)
    return values


def steps_kernel(
    blks,
    planes,
    own_tiles,
    left_scale,
    right_scale,
    beta_hbm,
    count_hbm,
    cols_hbm,
    u_hbm,
    v_hbm,
    tiles_hbm,
    left_hbm,
    right_hbm,
    out_ref,
    beta_s,
    count_s,
    cols_s,
    cols_v,
    u_scr,
    v_scr,
    tiles,
    left,
    right,
    left_t,
    right_t,
    v_send,
    v_all,
    v_table,
    cols_rows,
    put_hot,
    shift_scr,
    p_scr,
    contrib,
    gram_send,
    gram_recv,
    gram_sum,
    gram_all,
    gram_scr,
    diagonal,
    dot_send,
    dot_recv,
    part_send,
    part_recv,
    sent,
    copy_sem,
    send_sem,
    recv_sem,
):
    devices = blks * planes
    blocks, slots = cols_v.shape
    keep = left.shape[1]
    me_blk, me_plane = lax.axis_index("blk"), lax.axis_index("plane")
    me = me_blk * planes + me_plane
    chunks, rows = gram_send.shape[1:3]
    pad_tiles = v_send.shape[0]
    words = part_send.shape[1] - 1
    part_rows = 2 * words
    entries = contrib.shape[0]
    stride = entries // blocks
    two_power = blks & (blks - 1) == 0 and planes & (planes - 1) == 0
    unrolled = two_power and devices <= UNROLL_DEVICES
    if unrolled:
        blk_of, plane_of = flips(me_blk, blks), flips(me_plane, planes)
        order = far_first(blks, planes)

    def each_other(act):
        if unrolled:
            for b, p in order:
                act(blk_of[b] * planes + plane_of[p], (blk_of[b], plane_of[p]))
            return

        def body(step, carry):
            other = lax.rem(me + step, devices)
            act(other, (other // planes, lax.rem(other, planes)))
            return carry

        lax.fori_loop(1, devices, body, 0)

    owners = gram_all.shape[1]
    owner_blks = owners // planes
    first_owner = (blks - owner_blks) // 2
    owner = (me_blk >= first_owner) & (me_blk < first_owner + owner_blks)
    my_part = me - first_owner * planes

    barrier = pltpu.get_barrier_semaphore()
    each_other(
        lambda other, place: pl.semaphore_signal(
            barrier, inc=1, device_id=place, device_id_type=MESH
        )
    )

    pairs = (
        (v_hbm, v_scr),
        (cols_hbm, cols_v),
        (count_hbm, count_s),
        (cols_hbm, cols_s),
        (beta_hbm, beta_s),
        (u_hbm, u_scr),
        (left_hbm, left),
        (right_hbm, right),
        (tiles_hbm, tiles),
    )
    loads = [pltpu.make_async_copy(a, b, copy_sem.at[i]) for i, (a, b) in enumerate(pairs)]
    for load in loads:
        load.start()
    v_load, cols_load, count_load, index_load, beta_load, u_load, left_load, right_load, tiles_load = loads

    def send_one(phase, source, landing, place):
        pltpu.make_async_remote_copy(
            src_ref=source,
            dst_ref=landing,
            send_sem=send_sem.at[0],
            recv_sem=recv_sem.at[RECV[phase]],
            device_id=place,
            device_id_type=MESH,
        ).start()

    def send_all(phase, source, landing):
        each_other(lambda other, place: send_one(phase, source(other), landing.at[me], place))

    def wait_all(phase, landing):
        most = landing.at[pl.ds(0, devices - 1)]
        pltpu.make_async_copy(most, most, recv_sem.at[RECV[phase]]).wait()

    eye = lax.broadcasted_iota(jnp.int32, (LANES, LANES), 0) == lax.broadcasted_iota(
        jnp.int32, (LANES, LANES), 1
    )

    half = keep // 2
    half_row = lax.broadcasted_iota(jnp.int32, (half, keep), 0)
    half_lane = lax.broadcasted_iota(jnp.int32, (half, keep), 1)

    def to_col(row):
        return jnp.sum(jnp.where(eye, row, 0.0), axis=1, keepdims=True)

    def to_row(col):
        return jnp.sum(jnp.where(eye, col, 0.0), axis=0, keepdims=True)

    def fold(block):
        return jnp.sum(block.reshape(LANES // SUB, SUB, LANES), axis=0)

    v_load.wait()
    rounded = v_scr[...]
    if pad_tiles > own_tiles:
        rounded = jnp.concatenate(
            [rounded, jnp.zeros((pad_tiles - own_tiles, LANES), jnp.float32)], axis=0
        )
    rounded = rounded.astype(jnp.bfloat16)
    v_send[...] = rounded
    v_all[me] = rounded
    v_table[devices * pad_tiles :, :] = jnp.zeros((SUB, LANES), jnp.float32)

    def start_gram(side, basis_t):
        whole = basis_t[...]
        high = whole.astype(jnp.bfloat16)
        rest = whole - high.astype(jnp.float32)
        mid = rest.astype(jnp.bfloat16)
        low = (rest - mid.astype(jnp.float32)).astype(jnp.bfloat16)

        def product(a, b):
            return lax.dot_general(a, b, NT_DIMS, preferred_element_type=jnp.float32)

        cross = product(high, mid) + product(high, low)
        gram = product(high, high) + (cross + cross.T + product(mid, mid))
        top, low = gram[0:half, :], pltpu.roll(gram[half:, :], half, 1)
        folded = jnp.where(half_lane >= half_row, top, low)
        for c in range(chunks):
            gram_send[side, c] = folded[c * rows : (c + 1) * rows, :]
        diagonal[side] = jnp.sum(
            jnp.where(half_lane == half_row + half, gram[half:, :], 0.0), axis=0, keepdims=True
        )
        gram_recv[side, me] = gram_send[side, lax.rem(my_part + owners, chunks)]

    def send_gram(side, phase):
        def send(part, place):
            send_one(
                phase,
                gram_send.at[side, lax.rem(part, chunks)],
                gram_recv.at[side, me],
                place,
            )

        if unrolled:
            near = flips(lax.rem(me_blk, owner_blks), owner_blks)
            weight = lambda m: m[0] % 2 + m[1] // 2 + 0.3 * (m[1] % 2) + 0.6 * (m[0] // 2)
            pairs = [(k, p) for k in range(owner_blks) for p in range(planes)]
            for k, p in sorted(pairs, key=weight, reverse=True):
                part = near[k] * planes + plane_of[p]
                place = (first_owner + near[k], plane_of[p])
                if k == first_owner and p == 0:
                    pl.when(jnp.logical_not(owner))(functools.partial(send, part, place))
                else:
                    send(part, place)
            return

        def body(step, carry):
            part = lax.rem(me + step, owners)
            place = (first_owner + part // planes, lax.rem(part, planes))
            pl.when(part != my_part)(functools.partial(send, part, place))
            return carry

        lax.fori_loop(0, owners, body, 0)

    def share_gram(side, phase):
        @pl.when(owner)
        def _():
            wait_all(phase, gram_recv.at[side])
            mine = jnp.sum(gram_recv[side], axis=0)
            gram_sum[side] = mine
            gram_all[side, jnp.clip(my_part, 0, owners - 1)] = mine
            each_other(
                lambda other, place: send_one(
                    phase + 1, gram_sum.at[side], gram_all.at[side, my_part], place
                )
            )

    def wait_owned(phase, landing):
        for mine, size in ((owner, owners - 1), (jnp.logical_not(owner), owners)):
            if size:
                most = landing.at[pl.ds(0, size)]
                pl.when(mine)(pltpu.make_async_copy(most, most, recv_sem.at[RECV[phase]]).wait)

    def finish_gram(side, phase):
        wait_owned(phase + 1, gram_all.at[side])
        for c in range(chunks):
            gram_scr[c * rows : (c + 1) * rows, :] = gram_all[side, c]
        folded = gram_scr[...]
        strict = jnp.concatenate(
            [
                jnp.where(half_lane > half_row, folded, 0.0),
                pltpu.roll(jnp.where(half_lane < half_row, folded, 0.0), half, 1),
            ],
            axis=0,
        )
        main = jnp.sum(jnp.where(half_lane == half_row, folded, 0.0), axis=0, keepdims=True)
        return strict + strict.T + jnp.where(eye, main, 0.0)

    left_load.wait()
    for r in range(left.shape[0] // LANES):
        left_t[:, r * LANES : (r + 1) * LANES] = left[r * LANES : (r + 1) * LANES, :].T
    start_gram(0, left_t)

    pl.semaphore_wait(barrier, devices - 1)
    send_all(0, lambda other: v_send, v_all)
    send_gram(0, 1)

    cols_load.wait()
    count_load.wait()
    index_load.wait()
    beta_load.wait()
    u_load.wait()
    cols_rows[...] = jnp.full(cols_rows.shape, -1.0, jnp.float32)
    for r in range(blocks):
        row = cols_v[r : r + 1, :]
        alive = lax.broadcasted_iota(jnp.int32, (1, slots), 1) < count_s[r]
        cols_rows[r : r + 1, 0:slots] = jnp.where(alive, row, -1).astype(jnp.float32)
    lane = lax.broadcasted_iota(jnp.int32, (1, entries), 1)
    line = jnp.full((1, entries), -1.0, jnp.float32)
    for r in range(blocks):
        row = cols_rows[r : r + 1, :]
        if r:
            row = pltpu.roll(row, r * stride, 1)
        line = jnp.where((lane >= r * stride) & (lane < r * stride + slots), row, line)
    whole = line.astype(jnp.int32)
    put_row = jnp.where(whole < 0, -1, whole // own_tiles * part_rows + whole % own_tiles)
    hot = jnp.where(
        lax.broadcasted_iota(jnp.int32, (put_hot.shape[0], entries), 0) == put_row, 1.0, 0.0
    ).astype(jnp.bfloat16)
    put_hot[:, 0:entries] = hot
    put_hot[:, entries:] = hot
    contrib[...] = jnp.zeros_like(contrib)
    beta = beta_s[0]
    for r in range(blocks):
        shift_scr[r] = jnp.where(eye, -beta * u_scr[r : r + 1, :], 0.0)

    right_load.wait()
    for t in range(own_tiles):
        right_t[:, t * LANES : (t + 1) * LANES] = right[t * LANES : (t + 1) * LANES, :].T
    start_gram(1, right_t)
    tiles_load.wait()

    wait_all(0, v_all)
    v_table[0 : devices * pad_tiles, :] = (
        v_all[...].reshape(devices * pad_tiles, LANES).astype(jnp.float32)
    )
    for r in range(blocks):
        if r == blocks - 1:
            share_gram(0, 1)
        total = shift_scr[r]
        for s in range(slots):
            col = cols_s[r, s]
            if pad_tiles != own_tiles:
                col = col // own_tiles * pad_tiles + lax.rem(col, own_tiles)
            col = jnp.where(s < count_s[r], col, devices * pad_tiles)
            total = total + tiles[r, s].astype(jnp.float32) * v_table[pl.ds(col, 1), :]
        p_scr[r] = total
    dots = jnp.zeros((SUB, LANES), jnp.float32)
    square = jnp.zeros((SUB, LANES), jnp.float32)
    for r in range(blocks):
        p_col = jnp.broadcast_to(jnp.sum(p_scr[r], axis=1, keepdims=True), (LANES, LANES))
        p_scr[r] = p_col
        dots = dots + fold(left[r * LANES : (r + 1) * LANES, :] * p_col)
        square = square + fold(p_col * p_col)

    def start_dots(side, dots, square):
        lane = lax.broadcasted_iota(jnp.int32, (1, keep), 1)
        both = jnp.concatenate([dots, jnp.where(lane >= half, diagonal[side], square)], axis=0)
        dot_send[side] = both
        dot_recv[side, me] = both
        send_all(3 + side, lambda other: dot_send.at[side], dot_recv.at[side])

    def finish_dots(side, phase):
        gram = finish_gram(side, phase)
        wait_all(3 + side, dot_recv.at[side])
        both = jnp.sum(dot_recv[side], axis=0)
        first, square = both[0:1, :], both[1:2, 0:1]
        lane = lax.broadcasted_iota(jnp.int32, (1, keep), 1)
        gram = gram + jnp.where(eye & (lane >= half), both[1:2, :], 0.0)
        twice = jnp.where(eye, 2.0, 0.0) - gram
        coef = jnp.sum(twice * first, axis=1, keepdims=True)
        coef_row = to_row(coef)
        spread = jnp.sum(gram * coef, axis=0, keepdims=True)
        change = jnp.sum(coef_row * (spread - 2.0 * first), axis=1, keepdims=True)
        return coef, coef_row, square + change + 1e-06

    start_dots(
        0, jnp.sum(dots, axis=0, keepdims=True), jnp.sum(square, axis=0, keepdims=True)
    )
    pl.delay(1900)
    send_gram(1, 6)

    coef, coef_row, total = finish_dots(0, 1)
    inverse, alpha = lax.rsqrt(total), jnp.sqrt(total)

    for r in range(blocks):
        fix = jnp.sum(left[r * LANES : (r + 1) * LANES, :] * coef_row, axis=1, keepdims=True)
        p_scr[r] = (p_scr[r] - fix) * inverse

    spot = lax.broadcasted_iota(jnp.int32, (SUB, LANES), 0)
    for r in range(blocks):
        rounded = p_scr[r].astype(jnp.bfloat16)
        col = rounded.astype(jnp.float32)
        row = jnp.broadcast_to(to_row(col), (2 * SUB, LANES)).astype(jnp.bfloat16)
        for g in range(0, slots, SUB):
            lines = jnp.zeros((SUB, LANES), jnp.float32)
            for s in range(g, min(g + SUB, slots)):
                if s % SUB in ON_MXU:
                    line = jnp.dot(row, tiles[r, s], preferred_element_type=jnp.float32)[0:SUB, :]
                else:
                    line = jnp.sum(fold(tiles[r, s].astype(jnp.float32) * col), axis=0, keepdims=True)
                lines = jnp.where(spot == s - g, line, lines)
            contrib[r * stride + g : r * stride + g + SUB, :] = lines
    whole = contrib[...]
    high = whole.astype(jnp.bfloat16)
    low = (whole - high.astype(jnp.float32)).astype(jnp.bfloat16)
    spread = jnp.dot(
        put_hot[...], jnp.concatenate([high, low], axis=0), preferred_element_type=jnp.float32
    )
    parts = spread.reshape(devices, part_rows, LANES)
    top = jnp.maximum(jnp.max(jnp.abs(parts), axis=1, keepdims=True), 1e-30)
    power = jnp.floor(jnp.log2(top)) - 14.0
    whole = jnp.minimum(jnp.round(parts * jnp.exp2(-power)), 32767.0).astype(jnp.int32)
    part_send[:, 0:words, :] = lax.shift_left(whole[:, 0:words, :], 16) | (
        whole[:, words:, :] & 0xFFFF
    )
    part_send[:, words:, :] = power.astype(jnp.int32)
    part_recv[me] = part_send[me]
    send_all(5, lambda other: part_send.at[other], part_recv)
    for r in range(blocks):
        out_ref[own_tiles + r : own_tiles + r + 1, :] = to_row(p_scr[r]) * left_scale
    wait_all(5, part_recv)
    share_gram(1, 6)
    unit = jnp.exp2(part_recv[:, words:, :].astype(jnp.float32))
    word = part_recv[:, 0:words, :]
    halves = (lax.shift_right_arithmetic(word, 16), lax.shift_right_arithmetic(lax.shift_left(word, 16), 16))
    own = jnp.concatenate(
        [jnp.sum(half.astype(jnp.float32) * unit, axis=0) for half in halves], axis=0
    )
    r_vec = own[0:own_tiles, :] - alpha * v_scr[...]

    total = jnp.zeros((keep, LANES), jnp.float32)
    for t in range(own_tiles):
        total = total + right_t[:, t * LANES : (t + 1) * LANES] * r_vec[t : t + 1, :]
    dots = to_row(jnp.sum(total, axis=1, keepdims=True))
    square = jnp.sum(r_vec * r_vec, keepdims=True)
    start_dots(1, dots, jnp.broadcast_to(square, (1, LANES)))
    coef, coef_row, total = finish_dots(1, 6)
    beta_new = jnp.sqrt(total)
    place = lax.broadcasted_iota(jnp.int32, (1, LANES), 1)
    out_ref[own_tiles + blocks : own_tiles + blocks + 1, :] = jnp.where(
        place == 0, alpha, beta_new
    )
    inverse = right_scale * lax.rsqrt(total)
    for t in range(own_tiles):
        fix = jnp.sum(right_t[:, t * LANES : (t + 1) * LANES] * coef, axis=0, keepdims=True)
        out_ref[t : t + 1, :] = (r_vec[t : t + 1, :] - fix) * inverse

    each = v_send.shape[0] // 2 + 2 * dot_send.shape[1] + part_send.shape[1]
    grams = 2 * rows
    for mine, size in (
        (owner, (devices - 1) * (each + grams) + (owners - 1) * grams),
        (jnp.logical_not(owner), (devices - 1) * each + owners * grams),
    ):
        most = sent.at[pl.ds(0, size)]
        pl.when(mine)(pltpu.make_async_copy(most, most, send_sem.at[0]).wait)


def place_kernel(own_tiles, blocks, packed, out_left, out_right, out_coef):
    for r in range(blocks):
        out_left[:, r * LANES : (r + 1) * LANES] = packed[own_tiles + r : own_tiles + r + 1, :]
    for t in range(own_tiles):
        out_right[:, t * LANES : (t + 1) * LANES] = packed[t : t + 1, :]
    out_coef[...] = packed[own_tiles + blocks, 0:2]


def on_device(tiles, tile_cols, tile_count, u_start, v_start, beta_start, left_basis, right_basis):
    blks, planes = lax.axis_size("blk"), lax.axis_size("plane")
    devices = blks * planes
    blocks, slots = tile_cols.shape
    own_tiles = v_start.shape[0] // LANES
    left_rows, keep = left_basis.shape
    right_rows = right_basis.shape[0]
    pad_tiles = -(-own_tiles // 16) * 16
    part_rows = -(-own_tiles // 16) * 16
    owners = (blks // 2 if blks % 4 == 0 else blks) * planes
    rows = max(2, keep // 2 // owners)
    chunks = keep // 2 // rows
    stride = -(-slots // 8) * 8
    while (blocks * stride) % LANES:
        stride += 8
    entries = blocks * stride
    sent_rows = (devices - 1) * (pad_tiles // 2 + 4 + part_rows // 2 + 1 + 2 * rows)
    sent_rows += owners * 2 * rows
    f32, bf16, i32 = jnp.float32, jnp.bfloat16, jnp.int32
    vmem = pl.BlockSpec(memory_space=pltpu.VMEM)
    hbm = pl.BlockSpec(memory_space=pl.ANY)
    packed = pl.pallas_call(
        functools.partial(
            steps_kernel,
            blks,
            planes,
            own_tiles,
            math.sqrt(left_rows * devices),
            math.sqrt(right_rows * devices),
        ),
        out_shape=pltpu.VMEM((own_tiles + blocks + 1, LANES), f32),
        in_specs=[hbm] * 8,
        out_specs=vmem,
        scratch_shapes=[
            pltpu.SMEM((1,), f32),
            pltpu.SMEM((blocks,), i32),
            pltpu.SMEM((blocks, slots), i32),
            pltpu.VMEM((blocks, slots), i32),
            pltpu.VMEM((blocks, LANES), f32),
            pltpu.VMEM((own_tiles, LANES), f32),
            pltpu.VMEM(tiles.shape, bf16),
            pltpu.VMEM(left_basis.shape, f32),
            pltpu.VMEM(right_basis.shape, f32),
            pltpu.VMEM((keep, left_rows), f32),
            pltpu.VMEM((keep, right_rows), f32),
            pltpu.VMEM((pad_tiles, LANES), bf16),
            pltpu.VMEM((devices, pad_tiles, LANES), bf16),
            pltpu.VMEM((devices * pad_tiles + SUB, LANES), f32),
            pltpu.VMEM((-(-blocks // 8) * 8, entries), f32),
            pltpu.VMEM((devices * part_rows, 2 * entries), bf16),
            pltpu.VMEM((blocks, LANES, LANES), f32),
            pltpu.VMEM((blocks, LANES, LANES), f32),
            pltpu.VMEM((entries, LANES), f32),
            pltpu.VMEM((2, chunks, rows, keep), f32),
            pltpu.VMEM((2, devices, rows, keep), f32),
            pltpu.VMEM((2, rows, keep), f32),
            pltpu.VMEM((2, owners, rows, keep), f32),
            pltpu.VMEM((keep // 2, keep), f32),
            pltpu.VMEM((2, 1, keep), f32),
            pltpu.VMEM((2, 2, keep), f32),
            pltpu.VMEM((2, devices, 2, keep), f32),
            pltpu.VMEM((devices, part_rows // 2 + 1, LANES), i32),
            pltpu.VMEM((devices, part_rows // 2 + 1, LANES), i32),
            pltpu.VMEM((sent_rows, LANES), f32),
            pltpu.SemaphoreType.DMA((9,)),
            pltpu.SemaphoreType.DMA((1,)),
            pltpu.SemaphoreType.DMA((5,)),
        ],
        compiler_params=pltpu.CompilerParams(
            collective_id=0, has_side_effects=True, vmem_limit_bytes=MAIN_VMEM - 512 * (-(-(own_tiles + blocks + 1) // SUB) * SUB)
        ),
    )(
        beta_start,
        tile_count,
        tile_cols,
        u_start.reshape(blocks, LANES),
        v_start.reshape(own_tiles, LANES),
        tiles,
        left_basis,
        right_basis,
    )
    return pl.pallas_call(
        functools.partial(place_kernel, own_tiles, blocks),
        out_shape=(
            jax.ShapeDtypeStruct((1, left_rows), f32),
            jax.ShapeDtypeStruct((1, right_rows), f32),
            jax.ShapeDtypeStruct((2,), f32),
        ),
        in_specs=[vmem],
        out_specs=(vmem, vmem, vmem),
        compiler_params=pltpu.CompilerParams(vmem_limit_bytes=1048576),
    )(packed)


def solution(mesh):
    placed = (
        P(AXES, None, None, None),
        P(AXES, None),
        P(AXES),
        P(AXES),
        P(AXES),
        P(),
        P(AXES, None),
        P(AXES, None),
    )
    return jax.shard_map(
        on_device,
        mesh=mesh,
        in_specs=placed,
        out_specs=(P(None, AXES), P(None, AXES), P()),
        check_vma=False,
    )
```
